32 devices in a mesh: dp: 2 (over z, core), sp: 16 (over x, y).
Axes of the slice: x: 4, y: 4, z: 1, core: 2. Of those that a mesh axis runs over, the one named last changes fastest.
The devices are a block of a 4x4x8 slice.
Arguments:
- x: bfloat16 [4096, 4096], P(('dp', 'sp')), parts along dimension 0
- gain: bfloat16 [4096], replicated
- wq: bfloat16 [4096, 6144], replicated
- wk: bfloat16 [4096, 1024], replicated
- wv: bfloat16 [4096, 1024], replicated
- wo: bfloat16 [6144, 4096], replicated
Outputs:
- output: bfloat16 [4096, 4096], P(('dp', 'sp')), parts along dimension 0
There are 2 independent parts. The reference program is written for one: setup_inputs(seed, part) draws one part's arguments, and reference() takes and returns one part's arrays. A program takes and returns all parts, laid end to end along the dimension named above; an argument that names none is the same for every part.
All inputs are finite; a program needn't handle non-finite values.
Results may differ from the reference program's by a relative error of at most 0.012.
Values are sent between devices in bfloat16 or wider.
A program may use at most 768 MiB of HBM per device.

```python
import jax
import jax.numpy as jnp
from jax import lax

ROWS = 2048
D = 4096
HEADS = 48
KV_HEADS = 8
HEAD = 128
THETA = 10000


def setup_inputs(seed: int = 0, part: int = 0) -> dict:
    kx, kn, kq, kk, kv, ko = jax.random.split(jax.random.key(seed), 6)

    def weights(key, rows, columns):
        return jax.random.normal(key, (rows, columns), jnp.float32) * rows**-0.5

    drawn = {
        "x": jax.random.normal(jax.random.fold_in(kx, part), (ROWS, D), jnp.float32),
        "gain": 1 + 0.1 * jax.random.normal(kn, (D,), jnp.float32),
        "wq": 2 * weights(kq, D, HEADS * HEAD),
        "wk": 2 * weights(kk, D, KV_HEADS * HEAD),
        "wv": 4 * weights(kv, D, KV_HEADS * HEAD),
        "wo": weights(ko, HEADS * HEAD, D),
    }
    return {k: v.astype(jnp.bfloat16) for k, v in drawn.items()}


def normed(x, gain):
    wide = x.astype(jnp.float32)
    scale = lax.rsqrt(jnp.mean(wide * wide, -1, keepdims=True) + 1e-6)
    return (wide * scale * gain.astype(jnp.float32)).astype(jnp.bfloat16)


def turned(t, place, theta):
    half = t.shape[-1] // 2
    angle = place.astype(jnp.float32)[:, None] * theta ** (-jnp.arange(half, dtype=jnp.float32) / half)
    cos, sin = jnp.cos(angle)[:, None], jnp.sin(angle)[:, None]
    a, b = t[..., :half].astype(jnp.float32), t[..., half:].astype(jnp.float32)
    return jnp.concatenate([a * cos - b * sin, b * cos + a * sin], -1).astype(jnp.bfloat16)


def matmul(a, w):
    return jnp.dot(a, w, preferred_element_type=jnp.float32).astype(jnp.bfloat16)


def einsum(form, a, b):
    return jnp.einsum(form, a.astype(jnp.float32), b.astype(jnp.float32))


def attention(q, k, v):
    scores = einsum("tgsd,ugd->gstu", q, k) * q.shape[-1] ** -0.5
    token = jnp.arange(q.shape[0])
    scores = jnp.where(token[:, None] >= token, scores, -jnp.inf)
    weights = jax.nn.softmax(scores, -1).astype(jnp.bfloat16)
    return einsum("gstu,ugd->tgsd", weights, v).astype(jnp.bfloat16)


def reference(x, gain, wq, wk, wv, wo):
    a, place = normed(x, gain), jnp.arange(ROWS)
    q = turned(matmul(a, wq).reshape(ROWS, HEADS, HEAD), place, THETA).reshape(ROWS, KV_HEADS, -1, HEAD)
    k = turned(matmul(a, wk).reshape(ROWS, KV_HEADS, HEAD), place, THETA)
    v = matmul(a, wv).reshape(ROWS, KV_HEADS, HEAD)
    seen = attention(q, k, v).reshape(ROWS, HEADS * HEAD)
    return (x.astype(jnp.float32) + jnp.dot(seen, wo, preferred_element_type=jnp.float32)).astype(jnp.bfloat16)
```

```python
import functools
import math

import jax
import jax.numpy as jnp
from jax import lax
from jax.experimental import pallas as pl
from jax.experimental.pallas import tpu as pltpu
from jax.sharding import PartitionSpec as P

HEAD = 128
THETA = 10000
LOG2E = 1.4426950408889634
HIDDEN = -2e30
MESH = pl.DeviceIdType.MESH
TILE = 256
SLOTS = 5
WIDE = 1024
WO_SLOTS = 20


def _kernel(side, own, dim, group, x_hbm, gain_ref, cos_ref, sin_ref, wq, wk, wv, wo, out_hbm,
            x_s, a_s, w_s, wo_s, kv_snd, kv, q_snd, q, o_snd, o, y_s, out_s, s_s,
            x_sem, w_sem, wo_sem, out_sem, kv1_s, kv1_r, kv2_s, kv2_r, q_s, q_r, o_s, o_r):
    i = lax.axis_index("sp")
    x, y = lax.div(i, side), lax.rem(i, side)
    place = (x, y)
    chunk = group * HEAD
    per = chunk // TILE
    n_kv = 2 * (2 * side) * HEAD // TILE
    n_q = 2 * side * per
    n_wo = dim // WIDE
    e = HEAD**-0.5 * LOG2E

    def dev(px, py):
        return {"sp": px * side + py}

    def peer(kind, p):
        return dev(p, y) if kind == 0 else dev(x, p)

    barrier = pltpu.get_barrier_semaphore()
    for kind in range(2):
        for rel in range(1, side):
            pl.semaphore_signal(barrier, inc=1, device_id=peer(kind, lax.rem(place[kind] + rel, side)), device_id_type=MESH)

    def kv_tile(t):
        half = side * HEAD // TILE
        kind, r = divmod(t, 2 * half)
        what, c = divmod(r, half)
        return (wk, wv)[what].at[:, pl.ds((kind * half + c) * TILE, TILE)]

    def q_group(c):
        kind, rel = lax.div(c, side), lax.rem(lax.rem(c, side) + 1, side)
        p = lax.rem(jnp.where(kind == 0, x, y) + rel, side)
        return kind, rel, p, kind * side + p

    def q_tile(u):
        c, j = lax.div(u, per), lax.rem(u, per)
        _, _, _, g = q_group(c)
        return wq.at[:, pl.ds(pl.multiple_of(g * chunk + j * TILE, TILE), TILE)]

    def w_copy(src, slot):
        return pltpu.make_async_copy(src, w_s.at[slot], w_sem.at[slot])

    def wo_copy(w):
        g, c = lax.div(w, n_wo), lax.rem(w, n_wo)
        slot = lax.rem(w, WO_SLOTS)
        src = wo.at[pl.ds(pl.multiple_of(g * chunk, chunk), chunk), pl.ds(pl.multiple_of(c * WIDE, WIDE), WIDE)]
        return pltpu.make_async_copy(src, wo_s.at[slot], wo_sem.at[slot])

    x_copy = pltpu.make_async_copy(x_hbm, x_s, x_sem)
    x_copy.start()
    for t in range(SLOTS):
        w_copy(kv_tile(t), t).start()
    x_copy.wait()

    def norm(r, _):
        rows = pl.ds(pl.multiple_of(r * 16, 16), 16)
        wide = x_s[rows, :].astype(jnp.float32)
        scale = lax.rsqrt(jnp.mean(wide * wide, -1, keepdims=True) + 1e-6)
        a_s[rows, :] = (wide * scale * gain_ref[...].astype(jnp.float32)).astype(jnp.bfloat16)
        return 0

    lax.fori_loop(0, own // 16, norm, 0)

    def project(slot):
        return jnp.dot(a_s[...], w_s[slot], preferred_element_type=jnp.float32).astype(jnp.bfloat16)

    def turned(t):
        t = t.astype(jnp.float32)
        return (t * cos_ref[...] + pltpu.roll(t, HEAD // 2, 1) * sin_ref[...]).astype(jnp.bfloat16)

    def kv1(kind, p):
        return pltpu.make_async_remote_copy(
            src_ref=kv_snd.at[kind * side + p], dst_ref=kv.at[kind, x, y],
            send_sem=kv1_s.at[kind, p], recv_sem=kv1_r.at[kind, place[kind]], device_id=peer(kind, p), device_id_type=MESH)

    def kv1_in(kind, p):
        dst = kv.at[0, p, y] if kind == 0 else kv.at[1, x, p]
        return pltpu.make_async_remote_copy(
            src_ref=kv_snd.at[kind * side + p], dst_ref=dst,
            send_sem=kv1_s.at[kind, p], recv_sem=kv1_r.at[kind, p], device_id=peer(kind, p), device_id_type=MESH)

    half = side * HEAD // TILE
    heads = TILE // HEAD
    for t in range(n_kv):
        kind, r = divmod(t, 2 * half)
        what, c = divmod(r, half)
        w_copy(kv_tile(t), t % SLOTS).wait()
        d = project(t % SLOTS)
        for n in range(heads):
            h = kind * side + c * heads + n
            part = d[:, n * HEAD : (n + 1) * HEAD]
            kv_snd[h, what] = turned(part) if what == 0 else part.T
        nxt = t + SLOTS
        w_copy(kv_tile(nxt) if nxt < n_kv else q_tile(jnp.int32(nxt - n_kv)), nxt % SLOTS).start()
        if what == 1 and c == half - 1:
            if kind == 0:
                pl.semaphore_wait(barrier, 2 * (side - 1))
            kv[kind, x, y] = kv_snd[kind * side + place[kind]]
            for rel in range(1, side):
                kv1(kind, lax.rem(place[kind] + rel, side)).start()

    def kv2(kind, p):
        ref = kv.at[0, :, y] if kind == 0 else kv.at[1, x]
        return pltpu.make_async_remote_copy(
            src_ref=ref, dst_ref=ref, send_sem=kv2_s.at[kind, p], recv_sem=kv2_r.at[kind, place[1 - kind]],
            device_id=peer(1 - kind, p), device_id_type=MESH)

    def kv2_in(kind, p):
        ref = kv.at[0, :, p] if kind == 0 else kv.at[1, p]
        return pltpu.make_async_remote_copy(
            src_ref=ref, dst_ref=ref, send_sem=kv2_s.at[kind, p], recv_sem=kv2_r.at[kind, p],
            device_id=peer(1 - kind, p), device_id_type=MESH)

    def second_leg(kind):
        for rel in range(1, side):
            kv1_in(kind, lax.rem(place[kind] + rel, side)).wait_recv()
        for rel in range(1, side):
            p = lax.rem(place[1 - kind] + rel, side)
            if kind == 0:
                kv2(0, p).start()
            else:
                @pl.when(p > x)
                def _():
                    kv2(1, p).start()

    def q_out(c):
        kind, rel, p, g = q_group(c)
        at = jnp.where(kind == 0, x, y)
        px, py = jnp.where(kind == 0, p, x), jnp.where(kind == 0, y, p)
        return rel, pltpu.make_async_remote_copy(
            src_ref=q_snd.at[c], dst_ref=q.at[kind, at], send_sem=q_s.at[c], recv_sem=q_r.at[kind, at],
            device_id=dev(px, py), device_id_type=MESH)

    def queries(c, _):
        for j in range(per):
            u = c * per + j
            slot = lax.rem(u + n_kv, SLOTS)
            w_copy(q_tile(u), slot).wait()
            d = project(slot)
            for n in range(heads):
                q_snd[c, j * heads + n] = turned(d[:, n * HEAD : (n + 1) * HEAD])

            @pl.when(u + SLOTS < n_q)
            def _():
                w_copy(q_tile(u + SLOTS), slot).start()

            @pl.when(u + SLOTS == n_q)
            def _():
                for w in range(WO_SLOTS):
                    wo_copy(jnp.int32(w)).start()

        rel, copy = q_out(c)

        @pl.when(rel != 0)
        def _():
            copy.start()

        @pl.when(rel == 0)
        def _():
            kind = lax.div(c, side)
            q[kind, jnp.where(kind == 0, x, y)] = q_snd[c]

        @pl.when(c == 0)
        def _():
            second_leg(0)

        @pl.when(c == 1)
        def _():
            second_leg(1)

        return 0

    lax.fori_loop(0, 2 * side, queries, 0)

    span = side * own
    strip = 2 * own
    ones = jnp.ones((8, span), jnp.bfloat16)

    def o_out(kind, idx):
        px, py = jnp.where(kind == 0, idx, x), jnp.where(kind == 0, y, idx)
        return pltpu.make_async_remote_copy(
            src_ref=o_snd.at[kind, idx], dst_ref=o.at[kind * side + jnp.where(kind == 0, x, y)], send_sem=o_s.at[kind, idx],
            recv_sem=o_r.at[kind * side + jnp.where(kind == 0, x, y)], device_id=dev(px, py), device_id_type=MESH)

    def work(kind, idx, parts, off):
        def scores(n):
            rows = q[kind, idx, 2 * n : 2 * n + 2].reshape(strip, HEAD)
            top = None
            for kk in range(parts):
                keys = kv[kind, kk, :, 0].reshape(span, HEAD)
                s = lax.dot_general(keys, rows, (((1,), (1,)), ((), ())), preferred_element_type=jnp.float32)
                if kk == parts - 1:
                    token = lax.rem(lax.broadcasted_iota(jnp.int32, (1, strip), 1), own) + off
                    s = jnp.where(token >= lax.broadcasted_iota(jnp.int32, (span, strip), 0), s, HIDDEN)
                s_s[n % 2, pl.ds(kk * span, span), :] = s
                m = s.max(axis=0, keepdims=True)
                top = m if top is None else jnp.maximum(top, m)
            return top

        def finish(n, top):
            acc = None
            for kk in range(parts):
                p = jnp.exp2((s_s[n % 2, pl.ds(kk * span, span), :] - top) * e).astype(jnp.bfloat16)
                values = jnp.concatenate([kv[kind, kk, b, 1] for b in range(side)], axis=1)
                values = jnp.concatenate([values, ones], axis=0)
                part = jnp.dot(values, p, preferred_element_type=jnp.float32)
                acc = part if acc is None else acc + part
            res = acc[:HEAD] * (1 / acc[HEAD : HEAD + 1])
            for m in range(2):
                at = (2 * n + m) * HEAD
                o_snd[kind, idx, :, at : at + HEAD] = res[:, m * own : (m + 1) * own].T.astype(jnp.bfloat16)

        top = scores(0)
        for n in range(group // 2):
            nxt = scores(n + 1) if n + 1 < group // 2 else None
            finish(n, top)
            top = nxt

    def block(kind, idx, parts, off):
        for c in range(1, side + 1):
            @pl.when(parts == c)
            def _():
                work(kind, idx, c, off)

        mine = jnp.where(kind == 0, x, y)

        @pl.when(idx != mine)
        def _():
            o_out(kind, idx).start()

        @pl.when(idx == mine)
        def _():
            o[kind * side + mine] = o_snd[kind, idx]

    def arrived(kind):
        for rel in range(1, side):
            p = lax.rem(place[kind] + rel, side)
            pltpu.make_async_remote_copy(
                src_ref=q.at[kind, p], dst_ref=q.at[kind, p], send_sem=q_s.at[0], recv_sem=q_r.at[kind, p],
                device_id=peer(kind, p), device_id_type=MESH).wait_recv()
            p = lax.rem(place[1 - kind] + rel, side)
            if kind == 0:
                kv2_in(0, p).wait_recv()
            else:
                @pl.when(p < x)
                def _():
                    kv2_in(1, p).wait_recv()

    def attention(n, _):
        kind, r = lax.div(n, side), lax.rem(n, side)
        idx = jnp.where(kind == 0, side - 1 - r, r)

        @pl.when(n == 0)
        def _():
            arrived(0)

        @pl.when(n == side)
        def _():
            arrived(1)

        block(kind, idx, jnp.where(kind == 0, idx, x) + 1, own * jnp.where(kind == 0, y, idx))
        return 0

    lax.fori_loop(0, 2 * side, attention, 0)

    y_s[...] = x_s[...].astype(jnp.float32)

    def out_copy(c):
        at = pl.ds(c * WIDE, WIDE)
        return pltpu.make_async_copy(out_s.at[:, at], out_hbm.at[:, at], out_sem.at[c])

    def result(g, _):
        kind = lax.div(g, side)
        mine = jnp.where(kind == 0, x, y)
        p = lax.rem(g, side)

        @pl.when(p != mine)
        def _():
            pltpu.make_async_remote_copy(
                src_ref=o.at[g], dst_ref=o.at[g], send_sem=o_s.at[0, 0], recv_sem=o_r.at[g],
                device_id=dev(jnp.where(kind == 0, p, x), jnp.where(kind == 0, y, p)), device_id_type=MESH).wait_recv()

        for c in range(n_wo):
            w = g * n_wo + c
            at = slice(c * WIDE, (c + 1) * WIDE)
            wo_copy(w).wait()
            y_s[:, at] += jnp.dot(o[g], wo_s[lax.rem(w, WO_SLOTS)], preferred_element_type=jnp.float32)

            @pl.when(w + WO_SLOTS < 2 * side * n_wo)
            def _():
                wo_copy(w + WO_SLOTS).start()

            @pl.when(g == 2 * side - 1)
            def _():
                out_s[:, at] = y_s[:, at].astype(jnp.bfloat16)
                out_copy(c).start()
        return 0

    lax.fori_loop(0, 2 * side, result, 0)

    for kind in range(2):
        for rel in range(1, side):
            p = lax.rem(place[kind] + rel, side)
            kv1(kind, p).wait_send()
            o_out(kind, p).wait_send()
            p = lax.rem(place[1 - kind] + rel, side)
            if kind == 0:
                kv2(0, p).wait_send()
            else:
                @pl.when(p > x)
                def _():
                    kv2(1, p).wait_send()
    for c in range(2 * side):
        if c % side != side - 1:
            q_out(jnp.int32(c))[1].wait_send()
    for c in range(n_wo):
        out_copy(c).wait()


def solution(mesh):
    side = math.isqrt(mesh.shape["sp"])

    def step(x, gain, wq, wk, wv, wo):
        own, dim = x.shape
        group = wq.shape[1] // wk.shape[1]
        half = HEAD // 2
        place = lax.axis_index("sp") * own + jnp.arange(own)
        angle = place.astype(jnp.float32)[:, None] * THETA ** (-jnp.arange(half, dtype=jnp.float32) / half)
        cos, sin = jnp.cos(angle), jnp.sin(angle)
        cos, sin = jnp.concatenate([cos, cos], 1), jnp.concatenate([-sin, sin], 1)
        blocks, chunk, bf = 2 * side, group * HEAD, jnp.bfloat16
        dma = pltpu.SemaphoreType.DMA
        hbm, vmem = pl.BlockSpec(memory_space=pl.ANY), pl.BlockSpec(memory_space=pltpu.VMEM)
        return pl.pallas_call(
            functools.partial(_kernel, side, own, dim, group),
            out_shape=jax.ShapeDtypeStruct((own, dim), bf),
            in_specs=[hbm, vmem, vmem, vmem, hbm, hbm, hbm, hbm],
            out_specs=hbm,
            scratch_shapes=[
                pltpu.VMEM((own, dim), bf), pltpu.VMEM((own, dim), bf),
                pltpu.VMEM((SLOTS, dim, TILE), bf), pltpu.VMEM((WO_SLOTS, chunk, WIDE), bf),
                pltpu.VMEM((blocks, 2, HEAD, HEAD), bf), pltpu.VMEM((2, side, side, 2, HEAD, HEAD), bf),
                pltpu.VMEM((blocks, group, own, HEAD), bf), pltpu.VMEM((2, side, group, own, HEAD), bf),
                pltpu.VMEM((2, side, own, chunk), bf), pltpu.VMEM((blocks, own, chunk), bf),
                pltpu.VMEM((own, dim), jnp.float32), pltpu.VMEM((own, dim), bf),
                pltpu.VMEM((2, side * side * own, 2 * own), jnp.float32),
                dma, dma((SLOTS,)), dma((WO_SLOTS,)), dma((dim // WIDE,)),
                dma((2, side)), dma((2, side)), dma((2, side)), dma((2, side)),
                dma((blocks,)), dma((2, side)), dma((2, side)), dma((blocks,)),
            ],
            compiler_params=pltpu.CompilerParams(collective_id=0, has_side_effects=True, vmem_limit_bytes=67043328),
        )(x, gain[None], cos, sin, wq, wk, wv, wo)

    tokens, whole = P(("dp", "sp"), None), P(None, None)
    return jax.shard_map(
        step,
        mesh=mesh,
        in_specs=(tokens, P(None), whole, whole, whole, whole),
        out_specs=tokens,
        check_vma=False,
    )
```

```python
import functools
import math

import jax
import jax.numpy as jnp
import numpy as np
from jax import lax
from jax.experimental import pallas as pl
from jax.experimental.pallas import tpu as pltpu
from jax.sharding import PartitionSpec as P

HEAD = 128
THETA = 10000
LOG2E = 1.4426950408889634
HIDDEN = -2e30
MESH = pl.DeviceIdType.MESH
TILE = 256
SLOTS = 10
WIDE = 1024
KEPT = 5


def _kernel(side, own, dim, group, x_hbm, gain_hbm, turn_hbm, base_hbm, wq, wk, wv, wo, out_hbm,
            gain_s, turn_s, base_s, a_s, w_s, wo_s, kv_snd, kv, q_snd, q, o, y_s, s_s,
            in_sem, w_sem, wo_sem, wo2_sem, out_sem, kv1_s, kv1_r, kv2_s, kv2_r, q_s, q_r, o_s, o_r):
    i = lax.axis_index("sp")
    x, y = lax.div(i, side), lax.rem(i, side)
    place = (x, y)
    chunk = group * HEAD
    per = chunk // TILE
    n_kv = 2 * (2 * side) * HEAD // TILE
    n_q = 2 * side * per
    n_wo = dim // WIDE
    e = HEAD**-0.5 * LOG2E

    def dev(px, py):
        return {"sp": px * side + py}

    def peer(kind, p):
        return dev(p, y) if kind == 0 else dev(x, p)

    barrier = pltpu.get_barrier_semaphore()
    for kind in range(2):
        for rel in range(1, side):
            pl.semaphore_signal(barrier, inc=1, device_id=peer(kind, lax.rem(place[kind] + rel, side)), device_id_type=MESH)

    def kv_tile(t):
        half = side * HEAD // TILE
        kind, r = divmod(t, 2 * half)
        what, c = divmod(r, half)
        return (wk, wv)[what].at[:, pl.ds((kind * half + c) * TILE, TILE)]

    def q_group(c):
        kind, rel = lax.div(c, side), lax.rem(lax.rem(c, side) + 1, side)
        p = lax.rem(jnp.where(kind == 0, x, y) + rel, side)
        return kind, rel, p, kind * side + p

    def q_tile(u):
        c, j = lax.div(u, per), lax.rem(u, per)
        _, _, _, g = q_group(c)
        return wq.at[:, pl.ds(pl.multiple_of(g * chunk + j * TILE, TILE), TILE)]

    def w_copy(src, slot):
        return pltpu.make_async_copy(src, w_s.at[slot], w_sem.at[slot])

    def wo_copy(g, c):
        src = wo.at[pl.ds(g * chunk, chunk), pl.ds(c * WIDE, WIDE)]
        return pltpu.make_async_copy(src, wo_s.at[g, c], wo_sem.at[g, c])

    def wo2_place(b):
        fit = dim // chunk
        return lax.div(b, fit), pl.ds(pl.multiple_of(lax.rem(b, fit) * chunk, chunk), chunk)

    def wo2_copy(b):
        slot, rows = wo2_place(b)
        g, c = KEPT + lax.div(b, dim // TILE), lax.rem(b, dim // TILE)
        src = wo.at[pl.ds(pl.multiple_of(g * chunk, chunk), chunk), pl.ds(pl.multiple_of(c * TILE, TILE), TILE)]
        return pltpu.make_async_copy(src, w_s.at[slot, rows], wo2_sem.at[b])

    n_wo2 = (2 * side - KEPT) * (dim // TILE)

    small = [pltpu.make_async_copy(src, dst, in_sem.at[n])
             for n, (src, dst) in enumerate([(x_hbm, a_s), (gain_hbm, gain_s), (turn_hbm, turn_s), (base_hbm, base_s)])]
    for copy in small:
        copy.start()
    for t in range(2):
        w_copy(kv_tile(t), t).start()
    with jax.named_scope("xwait"):
        for copy in small:
            copy.wait()
    for t in range(2, SLOTS):
        w_copy(kv_tile(t) if t < n_kv else q_tile(jnp.int32(t - n_kv)), t).start()

    gain = jnp.concatenate([gain_s[n : n + 1, :].astype(jnp.float32) for n in range(dim // HEAD)], axis=1)

    def norm(r, _):
        rows = pl.ds(pl.multiple_of(r * 16, 16), 16)
        wide = a_s[rows, :].astype(jnp.float32)
        y_s[rows, :] = wide
        scale = lax.rsqrt(jnp.mean(wide * wide, -1, keepdims=True) + 1e-6)
        a_s[rows, :] = (wide * scale * gain).astype(jnp.bfloat16)
        return 0

    with jax.named_scope("norm"):
        lax.fori_loop(0, own // 16, norm, 0)

    cos_b, sin_b = base_s[0, pl.ds(i, 1), :], base_s[1, pl.ds(i, 1), :]
    cos_r, sin_r = turn_s[0], turn_s[1]
    sign = jnp.where(lax.broadcasted_iota(jnp.int32, (1, HEAD), 1) < HEAD // 2, -1.0, 1.0)
    turn_s[0] = cos_b * cos_r - sin_b * sin_r
    turn_s[1] = (sin_b * cos_r + cos_b * sin_r) * sign

    def project(slot):
        return jnp.dot(a_s[...], w_s[slot], preferred_element_type=jnp.float32).astype(jnp.bfloat16)

    def turned(t):
        t = t.astype(jnp.float32)
        return (t * turn_s[0] + pltpu.roll(t, HEAD // 2, 1) * turn_s[1]).astype(jnp.bfloat16)

    def kv1(kind, p):
        return pltpu.make_async_remote_copy(
            src_ref=kv_snd.at[kind * side + p], dst_ref=kv.at[kind, x, y],
            send_sem=kv1_s.at[kind, p], recv_sem=kv1_r.at[kind, place[kind]], device_id=peer(kind, p), device_id_type=MESH)

    def kv1_in(kind, p):
        dst = kv.at[0, p, y] if kind == 0 else kv.at[1, x, p]
        return pltpu.make_async_remote_copy(
            src_ref=kv_snd.at[kind * side + p], dst_ref=dst,
            send_sem=kv1_s.at[kind, p], recv_sem=kv1_r.at[kind, p], device_id=peer(kind, p), device_id_type=MESH)

    half = side * HEAD // TILE
    heads = TILE // HEAD
    for kind in range(2):
        mine = range(kind * 2 * half, (kind + 1) * 2 * half)
        with jax.named_scope(f"kvw{kind}"):
            for t in mine:
                w_copy(kv_tile(t), t).wait()
        for t in mine:
            what, c = divmod(t - mine[0], half)
            d = project(t)
            for n in range(heads):
                h = kind * side + c * heads + n
                part = d[:, n * HEAD : (n + 1) * HEAD]
                kv_snd[h, what] = turned(part) if what == 0 else part.T
        for t in mine:
            w_copy(q_tile(jnp.int32(t + SLOTS - n_kv)), t).start()
        if kind == 0:
            with jax.named_scope("barrier"):
                pl.semaphore_wait(barrier, 2 * (side - 1))
        kv[kind, x, y] = kv_snd[kind * side + place[kind]]
        for rel in range(1, side):
            kv1(kind, lax.rem(place[kind] + rel, side)).start()

    def kv2(kind, p):
        ref = kv.at[0, :, y] if kind == 0 else kv.at[1, x]
        return pltpu.make_async_remote_copy(
            src_ref=ref, dst_ref=ref, send_sem=kv2_s.at[kind, p], recv_sem=kv2_r.at[kind, place[1 - kind]],
            device_id=peer(1 - kind, p), device_id_type=MESH)

    def kv2_in(kind, p):
        ref = kv.at[0, :, p] if kind == 0 else kv.at[1, p]
        return pltpu.make_async_remote_copy(
            src_ref=ref, dst_ref=ref, send_sem=kv2_s.at[kind, p], recv_sem=kv2_r.at[kind, p],
            device_id=peer(1 - kind, p), device_id_type=MESH)

    def second_leg(kind):
        for rel in range(1, side):
            kv1_in(kind, lax.rem(place[kind] + rel, side)).wait_recv()
        for rel in range(1, side):
            p = lax.rem(place[1 - kind] + rel, side)
            if kind == 0:
                kv2(0, p).start()
            else:
                @pl.when(p > x)
                def _():
                    kv2(1, p).start()

    def q_out(c):
        kind, rel, p, g = q_group(c)
        at = jnp.where(kind == 0, x, y)
        px, py = jnp.where(kind == 0, p, x), jnp.where(kind == 0, y, p)
        return rel, pltpu.make_async_remote_copy(
            src_ref=q_snd.at[c], dst_ref=q.at[kind, at], send_sem=q_s.at[c], recv_sem=q_r.at[kind, at],
            device_id=dev(px, py), device_id_type=MESH)

    def queries(c, _):
        slots = [lax.rem(c * per + j + n_kv, SLOTS) for j in range(per)]
        with jax.named_scope("qw"):
            for j in range(per):
                w_copy(q_tile(c * per + j), slots[j]).wait()

        @pl.when(c == 1)
        @jax.named_scope("leg0")
        def _():
            second_leg(0)

        @pl.when(c == side - 1)
        @jax.named_scope("leg1")
        def _():
            second_leg(1)

        for j in range(per):
            d = project(slots[j])
            for n in range(heads):
                q_snd[c, j * heads + n] = turned(d[:, n * HEAD : (n + 1) * HEAD])

        rel, copy = q_out(c)

        @pl.when(rel != 0)
        def _():
            copy.start()

        @pl.when(rel == 0)
        def _():
            kind = lax.div(c, side)
            q[kind, jnp.where(kind == 0, x, y)] = q_snd[c]

        for j in range(per):
            u = c * per + j + SLOTS

            @pl.when(u < n_q)
            def _():
                w_copy(q_tile(u), slots[j]).start()

        @pl.when(c == (n_q - SLOTS) // per)
        def _():
            for g in range(KEPT):
                for n in range(n_wo):
                    wo_copy(g, n).start()
        return 0

    with jax.named_scope("queries"):
        lax.fori_loop(0, 2 * side, queries, 0)

    def rest(b, _):
        wo2_copy(b).start()
        return 0

    lax.fori_loop(0, n_wo2, rest, 0)

    with jax.named_scope("qsent"):
        for c in range(2 * side):
            if c % side != side - 1:
                q_out(jnp.int32(c))[1].wait_send()

    span = side * own
    strip = 2 * own
    ones = jnp.ones((8, span), jnp.bfloat16)

    def o_out(kind, idx):
        px, py = jnp.where(kind == 0, idx, x), jnp.where(kind == 0, y, idx)
        return pltpu.make_async_remote_copy(
            src_ref=q_snd.at[kind * side + idx], dst_ref=o.at[kind * side + jnp.where(kind == 0, x, y)], send_sem=o_s.at[kind, idx],
            recv_sem=o_r.at[kind * side + jnp.where(kind == 0, x, y)], device_id=dev(px, py), device_id_type=MESH)

    def work(kind, idx, parts, off):
        def scores(n, kk):
            rows = q[kind, idx, 2 * n : 2 * n + 2].reshape(strip, HEAD)
            keys = kv[kind, kk, :, 0].reshape(span, HEAD)
            s = lax.dot_general(keys, rows, (((1,), (1,)), ((), ())), preferred_element_type=jnp.float32)
            if kk == parts - 1:
                token = lax.rem(lax.broadcasted_iota(jnp.int32, (1, strip), 1), own) + off
                s = jnp.where(token >= lax.broadcasted_iota(jnp.int32, (span, strip), 0), s, HIDDEN)
            s_s[pl.ds(kk * span, span), :] = s
            return s.max(axis=0, keepdims=True)

        top = functools.reduce(jnp.maximum, [scores(0, kk) for kk in range(parts)])
        for n in range(group // 2):
            acc, tops = None, []
            for kk in range(parts):
                p = jnp.exp2((s_s[pl.ds(kk * span, span), :] - top) * e).astype(jnp.bfloat16)
                if n + 1 < group // 2:
                    tops.append(scores(n + 1, kk))
                values = jnp.concatenate([kv[kind, kk, b, 1] for b in range(side)], axis=1)
                values = jnp.concatenate([values, ones], axis=0)
                part = jnp.dot(values, p, preferred_element_type=jnp.float32)
                acc = part if acc is None else acc + part
            res = acc[:HEAD] * (1 / acc[HEAD : HEAD + 1])
            for m in range(2):
                q_snd[kind * side + idx, 2 * n + m] = res[:, m * own : (m + 1) * own].T.astype(jnp.bfloat16)
            if tops:
                top = functools.reduce(jnp.maximum, tops)

    def block(kind, idx, parts, off):
        for c in range(1, side + 1):
            @pl.when(parts == c)
            def _():
                with jax.named_scope(f"work{c}"):
                    work(kind, idx, c, off)

        mine = jnp.where(kind == 0, x, y)

        @pl.when(idx != mine)
        def _():
            o_out(kind, idx).start()

        @pl.when(idx == mine)
        def _():
            o[kind * side + mine] = q_snd[kind * side + idx]

    def arrived(kind):
        for rel in range(1, side):
            p = lax.rem(place[kind] + rel, side)
            with jax.named_scope(f"arrq{kind}"):
                pltpu.make_async_remote_copy(
                    src_ref=q.at[kind, p], dst_ref=q.at[kind, p], send_sem=q_s.at[0], recv_sem=q_r.at[kind, p],
                    device_id=peer(kind, p), device_id_type=MESH).wait_recv()
            p = lax.rem(place[1 - kind] + rel, side)
            with jax.named_scope(f"arrk{kind}"):
                if kind == 0:
                    kv2_in(0, p).wait_recv()
                else:
                    @pl.when(p < x)
                    def _():
                        kv2_in(1, p).wait_recv()

    def attention(n, _):
        kind, r = lax.div(n, side), lax.rem(n, side)
        idx = jnp.where(kind == 0, side - 1 - r, r)

        @pl.when(n == 0)
        def _():
            arrived(0)

        @pl.when(n == side)
        def _():
            arrived(1)

        block(kind, idx, jnp.where(kind == 0, idx, x) + 1, own * jnp.where(kind == 0, y, idx))
        return 0

    lax.fori_loop(0, 2 * side, attention, 0)

    def out_copy(c):
        at = pl.ds(c * WIDE, WIDE)
        return pltpu.make_async_copy(a_s.at[:, at], out_hbm.at[:, at], out_sem.at[c])

    def result(g):
        kind, p = divmod(g, side)
        mine = place[kind]

        @pl.when(p != mine)
        @jax.named_scope(f"owait{g}")
        def _():
            pltpu.make_async_remote_copy(
                src_ref=o.at[g], dst_ref=o.at[g], send_sem=o_s.at[0, 0], recv_sem=o_r.at[g],
                device_id=peer(kind, jnp.int32(p)), device_id_type=MESH).wait_recv()

        rows = jnp.concatenate([o[g, n] for n in range(group)], axis=1)
        for c in range(n_wo):
            at = slice(c * WIDE, (c + 1) * WIDE)
            with jax.named_scope(f"wow{g}"):
                if g < KEPT:
                    wo_copy(g, c).wait()
                else:
                    tiles = [jnp.int32((g - KEPT) * (dim // TILE) + c * (WIDE // TILE) + n) for n in range(WIDE // TILE)]
                    for b in tiles:
                        wo2_copy(b).wait()
            if g < KEPT:
                y_s[:, at] += jnp.dot(rows, wo_s[g, c], preferred_element_type=jnp.float32)
            else:
                for n, b in enumerate(tiles):
                    slot, some = wo2_place(b)
                    here = slice(c * WIDE + n * TILE, c * WIDE + (n + 1) * TILE)
                    y_s[:, here] += jnp.dot(rows, w_s[slot, some], preferred_element_type=jnp.float32)
            if g == 2 * side - 1:
                a_s[:, at] = y_s[:, at].astype(jnp.bfloat16)
                out_copy(c).start()

    for g in range(2 * side):
        result(g)

    ending = jax.named_scope("end")
    ending.__enter__()
    for kind in range(2):
        for rel in range(1, side):
            p = lax.rem(place[kind] + rel, side)
            kv1(kind, p).wait_send()
            o_out(kind, p).wait_send()
            p = lax.rem(place[1 - kind] + rel, side)
            if kind == 0:
                kv2(0, p).wait_send()
            else:
                @pl.when(p > x)
                def _():
                    kv2(1, p).wait_send()
    for c in range(n_wo):
        out_copy(c).wait()
    ending.__exit__(None, None, None)


def solution(mesh):
    side = math.isqrt(mesh.shape["sp"])

    def step(x, gain, wq, wk, wv, wo):
        own, dim = x.shape
        group = wq.shape[1] // wk.shape[1]
        half, places = HEAD // 2, mesh.shape["sp"]
        rate = np.tile(np.float32(THETA) ** (-np.arange(half, dtype=np.float32) / half), 2).astype(np.float64)

        def turns(tokens):
            angle = tokens[:, None] * rate
            return jnp.asarray(np.stack([np.cos(angle), np.sin(angle)]).astype(np.float32))

        turn, base = turns(np.arange(own)), turns(np.arange(places) * own)
        blocks, chunk, bf = 2 * side, group * HEAD, jnp.bfloat16
        dma = pltpu.SemaphoreType.DMA
        hbm = pl.BlockSpec(memory_space=pl.ANY)
        return pl.pallas_call(
            functools.partial(_kernel, side, own, dim, group),
            out_shape=jax.ShapeDtypeStruct((own, dim), bf),
            in_specs=[hbm] * 8,
            out_specs=hbm,
            scratch_shapes=[
                pltpu.VMEM((dim // HEAD, HEAD), bf), pltpu.VMEM((2, own, HEAD), jnp.float32), pltpu.VMEM((2, places, HEAD), jnp.float32),
                pltpu.VMEM((own, dim), bf), pltpu.VMEM((SLOTS, dim, TILE), bf), pltpu.VMEM((KEPT, dim // WIDE, chunk, WIDE), bf),
                pltpu.VMEM((blocks, 2, HEAD, HEAD), bf), pltpu.VMEM((2, side, side, 2, HEAD, HEAD), bf),
                pltpu.VMEM((blocks, group, own, HEAD), bf), pltpu.VMEM((2, side, group, own, HEAD), bf),
                pltpu.VMEM((blocks, group, own, HEAD), bf),
                pltpu.VMEM((own, dim), jnp.float32), pltpu.VMEM((side * side * own, 2 * own), jnp.float32),
                dma((4,)), dma((SLOTS,)), dma((KEPT, dim // WIDE)), dma(((blocks - KEPT) * (dim // TILE),)), dma((dim // WIDE,)),
                dma((2, side)), dma((2, side)), dma((2, side)), dma((2, side)),
                dma((blocks,)), dma((2, side)), dma((2, side)), dma((blocks,)),
            ],
            compiler_params=pltpu.CompilerParams(collective_id=0, has_side_effects=True, vmem_limit_bytes=67043328),
        )(x, gain.reshape(dim // HEAD, HEAD), turn, base, wq, wk, wv, wo)

    tokens, whole = P(("dp", "sp"), None), P(None, None)
    return jax.shard_map(
        step,
        mesh=mesh,
        in_specs=(tokens, P(None), whole, whole, whole, whole),
        out_specs=tokens,
        check_vma=False,
    )
```

```python
import functools
import math

import jax
import jax.numpy as jnp
import numpy as np
from jax import lax
from jax.experimental import pallas as pl
from jax.experimental.pallas import tpu as pltpu
from jax.sharding import PartitionSpec as P

HEAD = 128
THETA = 10000
LOG2E = 1.4426950408889634
HIDDEN = -2e30
MESH = pl.DeviceIdType.MESH
TILE = 256
SLOTS = 10
EARLY = 3


def _kernel(side, own, dim, group, x_hbm, gain_hbm, turn_hbm, base_hbm, wq, wk, wv, wo, out_hbm,
            gain_s, turn_s, base_s, a_s, w_s, wo_a, wo_b, kv_snd, kv, q_snd, q, o, s_s,
            in_sem, w_sem, wo_sem, wo2_sem, out_sem, kv1_s, kv1_r, kv2_s, kv2_r, q_s, q_r, o_s, o_r):
    i = lax.axis_index("sp")
    x, y = lax.div(i, side), lax.rem(i, side)
    place = (x, y)
    chunk = group * HEAD
    per = chunk // TILE
    n_kv = 2 * (2 * side) * HEAD // TILE
    n_q = 2 * side * per
    strips = dim // TILE
    early = EARLY * chunk
    late = 2 * side * chunk - early
    e = HEAD**-0.5 * LOG2E

    def dev(px, py):
        return {"sp": px * side + py}

    def peer(kind, p):
        return dev(p, y) if kind == 0 else dev(x, p)

    barrier = pltpu.get_barrier_semaphore()
    for kind in range(2):
        for rel in range(1, side):
            pl.semaphore_signal(barrier, inc=1, device_id=peer(kind, lax.rem(place[kind] + rel, side)), device_id_type=MESH)

    def kv_tile(t):
        half = side * HEAD // TILE
        kind, r = divmod(t, 2 * half)
        what, c = divmod(r, half)
        return (wk, wv)[what].at[:, pl.ds((kind * half + c) * TILE, TILE)]

    def q_group(c):
        kind, rel = lax.div(c, side), lax.rem(lax.rem(c, side) + 1, side)
        p = lax.rem(jnp.where(kind == 0, x, y) + rel, side)
        return kind, rel, p, kind * side + p

    def q_tile(u):
        c, j = lax.div(u, per), lax.rem(u, per)
        _, _, _, g = q_group(c)
        return wq.at[:, pl.ds(pl.multiple_of(g * chunk + j * TILE, TILE), TILE)]

    def w_copy(src, slot):
        return pltpu.make_async_copy(src, w_s.at[slot], w_sem.at[slot])

    def wo_early(c):
        at = pl.ds(c * (dim // 8), dim // 8)
        return pltpu.make_async_copy(wo.at[pl.ds(0, early), at], wo_a.at[:, at], wo_sem.at[c])

    def wo_late(c):
        return w_s.at[c, pl.ds(0, late)] if c < SLOTS else wo_b.at[c - SLOTS]

    def wo_late_copy(c):
        return pltpu.make_async_copy(wo.at[pl.ds(early, late), pl.ds(c * TILE, TILE)], wo_late(c), wo2_sem.at[c])

    small = [pltpu.make_async_copy(src, dst, in_sem.at[n])
             for n, (src, dst) in enumerate([(x_hbm, a_s), (gain_hbm, gain_s), (turn_hbm, turn_s), (base_hbm, base_s)])]
    for copy in small:
        copy.start()
    for t in range(4):
        w_copy(kv_tile(t), t).start()
    with jax.named_scope("xwait"):
        for copy in small:
            copy.wait()
    for t in range(4, SLOTS):
        w_copy(kv_tile(t) if t < n_kv else q_tile(jnp.int32(t - n_kv)), t).start()

    gain = jnp.concatenate([gain_s[n : n + 1, :].astype(jnp.float32) for n in range(dim // HEAD)], axis=1)

    def norm(r, _):
        rows = pl.ds(pl.multiple_of(r * 16, 16), 16)
        wide = a_s[rows, :].astype(jnp.float32)
        scale = lax.rsqrt(jnp.mean(wide * wide, -1, keepdims=True) + 1e-6)
        a_s[rows, :] = (wide * scale * gain).astype(jnp.bfloat16)
        return 0

    with jax.named_scope("norm"):
        lax.fori_loop(0, own // 16, norm, 0)

    cos_b, sin_b = base_s[0, pl.ds(i, 1), :], base_s[1, pl.ds(i, 1), :]
    cos_r, sin_r = turn_s[0], turn_s[1]
    sign = jnp.where(lax.broadcasted_iota(jnp.int32, (1, HEAD), 1) < HEAD // 2, -1.0, 1.0)
    turn_s[0] = cos_b * cos_r - sin_b * sin_r
    turn_s[1] = (sin_b * cos_r + cos_b * sin_r) * sign

    def project(slot):
        return jnp.dot(a_s[...], w_s[slot], preferred_element_type=jnp.float32).astype(jnp.bfloat16)

    def turned(t):
        t = t.astype(jnp.float32)
        return (t * turn_s[0] + pltpu.roll(t, HEAD // 2, 1) * turn_s[1]).astype(jnp.bfloat16)

    def kv1(kind, p):
        return pltpu.make_async_remote_copy(
            src_ref=kv_snd.at[kind * side + p], dst_ref=kv.at[kind, x, y],
            send_sem=kv1_s.at[kind, p], recv_sem=kv1_r.at[kind, place[kind]], device_id=peer(kind, p), device_id_type=MESH)

    def kv1_in(kind, p):
        dst = kv.at[0, p, y] if kind == 0 else kv.at[1, x, p]
        return pltpu.make_async_remote_copy(
            src_ref=kv_snd.at[kind * side + p], dst_ref=dst,
            send_sem=kv1_s.at[kind, p], recv_sem=kv1_r.at[kind, p], device_id=peer(kind, p), device_id_type=MESH)

    half = side * HEAD // TILE
    heads = TILE // HEAD
    for kind in range(2):
        mine = range(kind * 2 * half, (kind + 1) * 2 * half)
        with jax.named_scope(f"kvw{kind}"):
            for t in mine:
                w_copy(kv_tile(t), t).wait()
        for t in mine:
            what, c = divmod(t - mine[0], half)
            d = project(t)
            for n in range(heads):
                h = kind * side + c * heads + n
                part = d[:, n * HEAD : (n + 1) * HEAD]
                kv_snd[h, what] = turned(part) if what == 0 else part.T
        for t in mine:
            w_copy(q_tile(jnp.int32(t + SLOTS - n_kv)), t).start()
        if kind == 0:
            with jax.named_scope("barrier"):
                pl.semaphore_wait(barrier, 2 * (side - 1))
        kv[kind, x, y] = kv_snd[kind * side + place[kind]]
        for rel in range(1, side):
            kv1(kind, lax.rem(place[kind] + rel, side)).start()

    def kv2(kind, p, part, to, sem):
        some = pl.ds(part * (side // 2), side // 2)
        ref = kv.at[0, some, p] if kind == 0 else kv.at[1, p, some]
        return pltpu.make_async_remote_copy(
            src_ref=ref, dst_ref=ref, send_sem=kv2_s.at[kind, sem], recv_sem=kv2_r.at[kind, p, part],
            device_id=peer(1 - kind, to), device_id_type=MESH)

    up, down = [lax.rem(p + 1, side) for p in (y, x)], [lax.rem(p + side - 1, side) for p in (y, x)]
    direct_a = [kv2(0, y, 0, up[0], 0), kv2(0, y, 1, down[0], 2), kv2(0, y, 1, up[0], 1), kv2(0, y, 0, down[0], 3)]
    relay_a = [kv2(0, down[0], 0, up[0], 4), kv2(0, up[0], 1, down[0], 5)]
    direct_b = [kv2(1, x, part, up[1], part) for part in range(2)]
    around_b = [kv2(1, x, part, down[1], 2 + part) for part in range(2)]
    relay_b = [kv2(1, jnp.where(x == side - 1, 0, x - 1), part, 2 * side - 3 - x, 4 + part) for part in range(2)]

    def second_leg(kind):
        for rel in range(1, side):
            kv1_in(kind, lax.rem(place[kind] + rel, side)).wait_recv()
        if kind == 0:
            for copy in direct_a:
                copy.start()
        else:
            @pl.when(x < side - 1)
            def _():
                for copy in direct_b:
                    copy.start()

            @pl.when(x == 0)
            def _():
                for copy in around_b:
                    copy.start()

    def pass_on_a():
        for copy in relay_a:
            copy.wait_recv()
            copy.start()

    def pass_on_b(part):
        @pl.when(x >= side - 2)
        def _():
            relay_b[part].wait_recv()
            relay_b[part].start()

    def q_out(c):
        kind, rel, p, g = q_group(c)
        at = jnp.where(kind == 0, x, y)
        px, py = jnp.where(kind == 0, p, x), jnp.where(kind == 0, y, p)
        return rel, pltpu.make_async_remote_copy(
            src_ref=q_snd.at[c], dst_ref=q.at[kind, at], send_sem=q_s.at[c], recv_sem=q_r.at[kind, at],
            device_id=dev(px, py), device_id_type=MESH)

    def queries(c, _):
        slots = [lax.rem(c * per + j + n_kv, SLOTS) for j in range(per)]
        with jax.named_scope("qw"):
            for j in range(per):
                w_copy(q_tile(c * per + j), slots[j]).wait()

        @pl.when(c == 2 * side - 2)
        def _():
            wo_early(0).start()

        @pl.when(c == 2 * side - 1)
        def _():
            for n in range(1, 8):
                wo_early(n).start()

        @pl.when(c == 1)
        @jax.named_scope("leg0")
        def _():
            second_leg(0)

        @pl.when(c == side - 1)
        @jax.named_scope("leg1")
        def _():
            second_leg(1)

        @pl.when(c == side)
        @jax.named_scope("pass0")
        def _():
            pass_on_a()

        @pl.when(c == 2 * side - 1)
        @jax.named_scope("pass1")
        def _():
            pass_on_b(0)

        for j in range(per):
            d = project(slots[j])
            for n in range(heads):
                q_snd[c, j * heads + n] = turned(d[:, n * HEAD : (n + 1) * HEAD])

        rel, copy = q_out(c)

        @pl.when(rel != 0)
        def _():
            copy.start()

        @pl.when(rel == 0)
        def _():
            kind = lax.div(c, side)
            q[kind, jnp.where(kind == 0, x, y)] = q_snd[c]

        for j in range(per):
            u = c * per + j + SLOTS

            @pl.when(u < n_q)
            def _():
                w_copy(q_tile(u), slots[j]).start()

        return 0

    with jax.named_scope("queries"):
        lax.fori_loop(0, 2 * side, queries, 0)

    again = pltpu.make_async_copy(x_hbm, a_s, in_sem.at[0])
    again.start()

    with jax.named_scope("pass2"):
        pass_on_b(1)

    span = side * own
    strip = 2 * own
    ones = jnp.ones((8, span), jnp.bfloat16)

    def o_out(kind, idx):
        px, py = jnp.where(kind == 0, idx, x), jnp.where(kind == 0, y, idx)
        return pltpu.make_async_remote_copy(
            src_ref=q_snd.at[kind * side + idx], dst_ref=o.at[kind * side + jnp.where(kind == 0, x, y)], send_sem=o_s.at[kind, idx],
            recv_sem=o_r.at[kind * side + jnp.where(kind == 0, x, y)], device_id=dev(px, py), device_id_type=MESH)

    def work(kind, idx, parts, off):
        def scores(n):
            rows = q[kind, idx, 2 * n : 2 * n + 2].reshape(strip, HEAD)
            top = None
            for kk in range(parts):
                keys = kv[kind, kk, :, 0].reshape(span, HEAD)
                s = lax.dot_general(keys, rows, (((1,), (1,)), ((), ())), preferred_element_type=jnp.float32)
                if kk == parts - 1:
                    token = lax.rem(lax.broadcasted_iota(jnp.int32, (1, strip), 1), own) + off
                    s = jnp.where(token >= lax.broadcasted_iota(jnp.int32, (span, strip), 0), s, HIDDEN)
                s_s[n % 2, pl.ds(kk * span, span), :] = s
                m = s.max(axis=0, keepdims=True)
                top = m if top is None else jnp.maximum(top, m)
            return top

        def finish(n, top):
            acc = None
            for kk in range(parts):
                p = jnp.exp2((s_s[n % 2, pl.ds(kk * span, span), :] - top) * e).astype(jnp.bfloat16)
                values = jnp.concatenate([kv[kind, kk, b, 1] for b in range(side)], axis=1)
                values = jnp.concatenate([values, ones], axis=0)
                part = jnp.dot(values, p, preferred_element_type=jnp.float32)
                acc = part if acc is None else acc + part
            res = acc[:HEAD] * (1 / acc[HEAD : HEAD + 1])
            for m in range(2):
                q_snd[kind * side + idx, 2 * n + m] = res[:, m * own : (m + 1) * own].T.astype(jnp.bfloat16)

        top = scores(0)
        for n in range(group // 2):
            nxt = scores(n + 1) if n + 1 < group // 2 else None
            finish(n, top)
            top = nxt

    def block(kind, idx, parts, off):
        for c in range(1, side + 1):
            @pl.when(parts == c)
            def _():
                with jax.named_scope(f"work{c}"):
                    work(kind, idx, c, off)

        mine = jnp.where(kind == 0, x, y)

        @pl.when(idx != mine)
        def _():
            o_out(kind, idx).start()

        @pl.when(idx == mine)
        def _():
            o[kind * side + mine] = q_snd[kind * side + idx]

    def arrived(kind):
        for rel in range(1, side):
            p = lax.rem(place[kind] + rel, side)
            with jax.named_scope(f"arrq{kind}"):
                pltpu.make_async_remote_copy(
                    src_ref=q.at[kind, p], dst_ref=q.at[kind, p], send_sem=q_s.at[0], recv_sem=q_r.at[kind, p],
                    device_id=peer(kind, p), device_id_type=MESH).wait_recv()
        with jax.named_scope(f"arrk{kind}"):
            if kind == 0:
                across = lax.rem(y + 2, side)
                for p, part in [(down[0], 1), (up[0], 0), (across, 0), (across, 1)]:
                    kv2(0, p, part, p, 0).wait_recv()
            else:
                for part in range(2):
                    @pl.when((x == 1) | (x == 2))
                    def _():
                        kv2(1, 0, part, 0, 0).wait_recv()

                    @pl.when(x == side - 1)
                    def _():
                        kv2(1, 1, part, 1, 0).wait_recv()
                        kv2(1, 2, part, 2, 0).wait_recv()
        with jax.named_scope(f"qsent{kind}"):
            for c in range(kind * side, (kind + 1) * side - 1):
                q_out(jnp.int32(c))[1].wait_send()

    def attention(n, _):
        kind, r = lax.div(n, side), lax.rem(n, side)
        idx = lax.rem(jnp.where(kind == 0, x, y) + r + 1, side)

        for m in range(side):
            @pl.when(n == m)
            def _():
                for c in range(m * strips // side, (m + 1) * strips // side):
                    wo_late_copy(strips - 1 - c).start()

        @pl.when(n == 0)
        def _():
            arrived(0)

        @pl.when(n == side)
        def _():
            arrived(1)

        block(kind, idx, jnp.where(kind == 0, idx, x) + 1, own * jnp.where(kind == 0, y, idx))
        return 0

    lax.fori_loop(0, 2 * side, attention, 0)

    def out_copy(c):
        at = pl.ds(c * (dim // 4), dim // 4)
        return pltpu.make_async_copy(a_s.at[:, at], out_hbm.at[:, at], out_sem.at[c])

    def wait_o(g):
        kind, p = divmod(g, side)

        @pl.when(p != place[kind])
        @jax.named_scope(f"owait{g}")
        def _():
            pltpu.make_async_remote_copy(
                src_ref=o.at[g], dst_ref=o.at[g], send_sem=o_s.at[0, 0], recv_sem=o_r.at[g],
                device_id=peer(kind, jnp.int32(p)), device_id_type=MESH).wait_recv()

    def rows_of(groups):
        return jnp.concatenate([o[g, n] for g in groups for n in range(group)], axis=1)

    for g in range(EARLY):
        wait_o(g)
    with jax.named_scope("woa"):
        for c in range(8):
            wo_early(c).wait()
    rows = rows_of(range(EARLY))
    for c in range(strips):
        s_s[0, pl.ds(c * own, own), :] = jnp.dot(rows, wo_a[:, c * TILE : (c + 1) * TILE], preferred_element_type=jnp.float32)
    again.wait()
    for g in range(EARLY, 2 * side):
        wait_o(g)
    rows = rows_of(range(EARLY, 2 * side))
    order = [strips - 1 - c for c in range(strips)]
    for n in range(4):
        some = order[n * strips // 4 : (n + 1) * strips // 4]
        with jax.named_scope(f"wob{n}"):
            for c in some:
                wo_late_copy(c).wait()
        for c in some:
            at = slice(c * TILE, (c + 1) * TILE)
            tile = w_s[c, pl.ds(0, late), :] if c < SLOTS else wo_b[c - SLOTS]
            part = s_s[0, pl.ds(c * own, own), :] + jnp.dot(rows, tile, preferred_element_type=jnp.float32)
            a_s[:, at] = (a_s[:, at].astype(jnp.float32) + part).astype(jnp.bfloat16)
        out_copy(3 - n).start()

    ending = jax.named_scope("end")
    ending.__enter__()
    for kind in range(2):
        for rel in range(1, side):
            p = lax.rem(place[kind] + rel, side)
            kv1(kind, p).wait_send()
            o_out(kind, p).wait_send()
    for copy in direct_a + relay_a:
        copy.wait_send()

    @pl.when(x < side - 1)
    def _():
        for copy in direct_b:
            copy.wait_send()

    @pl.when(x == 0)
    def _():
        for copy in around_b:
            copy.wait_send()

    @pl.when(x >= side - 2)
    def _():
        for copy in relay_b:
            copy.wait_send()

    for c in range(4):
        out_copy(c).wait()
    ending.__exit__(None, None, None)


def solution(mesh):
    side = math.isqrt(mesh.shape["sp"])

    def step(x, gain, wq, wk, wv, wo):
        own, dim = x.shape
        group = wq.shape[1] // wk.shape[1]
        half, places = HEAD // 2, mesh.shape["sp"]
        rate = np.tile(np.float32(THETA) ** (-np.arange(half, dtype=np.float32) / half), 2).astype(np.float64)

        def turns(tokens):
            angle = tokens[:, None] * rate
            return jnp.asarray(np.stack([np.cos(angle), np.sin(angle)]).astype(np.float32))

        turn, base = turns(np.arange(own)), turns(np.arange(places) * own)
        blocks, chunk, bf = 2 * side, group * HEAD, jnp.bfloat16
        dma = pltpu.SemaphoreType.DMA
        hbm = pl.BlockSpec(memory_space=pl.ANY)
        return pl.pallas_call(
            functools.partial(_kernel, side, own, dim, group),
            out_shape=jax.ShapeDtypeStruct((own, dim), bf),
            in_specs=[hbm] * 8,
            out_specs=hbm,
            scratch_shapes=[
                pltpu.VMEM((dim // HEAD, HEAD), bf), pltpu.VMEM((2, own, HEAD), jnp.float32), pltpu.VMEM((2, places, HEAD), jnp.float32),
                pltpu.VMEM((own, dim), bf), pltpu.VMEM((SLOTS, dim, TILE), bf),
                pltpu.VMEM((EARLY * chunk, dim), bf), pltpu.VMEM((dim // TILE - SLOTS, (blocks - EARLY) * chunk, TILE), bf),
                pltpu.VMEM((blocks, 2, HEAD, HEAD), bf), pltpu.VMEM((2, side, side, 2, HEAD, HEAD), bf),
                pltpu.VMEM((blocks, group, own, HEAD), bf), pltpu.VMEM((2, side, group, own, HEAD), bf),
                pltpu.VMEM((blocks, group, own, HEAD), bf),
                pltpu.VMEM((2, side * side * own, 2 * own), jnp.float32),
                dma((4,)), dma((SLOTS,)), dma((8,)), dma((dim // TILE,)), dma((4,)),
                dma((2, side)), dma((2, side)), dma((2, 6)), dma((2, side, 2)),
                dma((blocks,)), dma((2, side)), dma((2, side)), dma((blocks,)),
            ],
            compiler_params=pltpu.CompilerParams(collective_id=0, has_side_effects=True, vmem_limit_bytes=67043328),
        )(x, gain.reshape(dim // HEAD, HEAD), turn, base, wq, wk, wv, wo)

    tokens, whole = P(("dp", "sp"), None), P(None, None)
    return jax.shard_map(
        step,
        mesh=mesh,
        in_specs=(tokens, P(None), whole, whole, whole, whole),
        out_specs=tokens,
        check_vma=False,
    )
```

```python
import functools
import math

import jax
import jax.numpy as jnp
import numpy as np
from jax import lax
from jax.experimental import pallas as pl
from jax.experimental.pallas import tpu as pltpu
from jax.sharding import PartitionSpec as P

HEAD = 128
THETA = 10000
LOG2E = 1.4426950408889634
HIDDEN = -2e30
MESH = pl.DeviceIdType.MESH
TILE = 256
SLOTS = 10
EARLY = 3


def _kernel(side, own, dim, group, x_hbm, gain_hbm, turn_hbm, base_hbm, wq, wk, wv, wo, out_hbm,
            gain_s, turn_s, base_s, a_s, w_s, wo_a, wo_b, kv_snd, kv, q_snd, q, o, s_s,
            in_sem, w_sem, wo_sem, wo2_sem, out_sem, kv1_s, kv1_r, kv2_s, kv2_r, q_s, q_r, o_s, o_r):
    i = lax.axis_index("sp")
    x, y = lax.div(i, side), lax.rem(i, side)
    place = (x, y)
    chunk = group * HEAD
    per = chunk // TILE
    n_kv = 2 * (2 * side) * HEAD // TILE
    n_q = 2 * side * per
    strips = dim // TILE
    early = EARLY * chunk
    late = 2 * side * chunk - early
    e = HEAD**-0.5 * LOG2E

    def dev(px, py):
        return {"sp": px * side + py}

    def peer(kind, p):
        return dev(p, y) if kind == 0 else dev(x, p)

    barrier = pltpu.get_barrier_semaphore()
    for kind in range(2):
        for rel in range(1, side):
            pl.semaphore_signal(barrier, inc=1, device_id=peer(kind, lax.rem(place[kind] + rel, side)), device_id_type=MESH)

    def kv_tile(t):
        half = side * HEAD // TILE
        kind, r = divmod(t, 2 * half)
        what, c = divmod(r, half)
        return (wk, wv)[what].at[:, pl.ds((kind * half + c) * TILE, TILE)]

    def q_group(c):
        kind, s = lax.div(c, side), lax.rem(c, side)
        rel = jnp.where(s == 0, 2, jnp.where(s == 1, 1, lax.rem(s + 1, side)))
        p = lax.rem(jnp.where(kind == 0, x, y) + rel, side)
        return kind, rel, p, kind * side + p

    def q_tile(u):
        c, j = lax.div(u, per), lax.rem(u, per)
        _, _, _, g = q_group(c)
        return wq.at[:, pl.ds(pl.multiple_of(g * chunk + j * TILE, TILE), TILE)]

    def w_copy(src, slot):
        return pltpu.make_async_copy(src, w_s.at[slot], w_sem.at[slot])

    def wo_early(c):
        at = pl.ds(c * (dim // 8), dim // 8)
        return pltpu.make_async_copy(wo.at[pl.ds(0, early), at], wo_a.at[:, at], wo_sem.at[c])

    def wo_late(c):
        return w_s.at[c, pl.ds(0, late)] if c < SLOTS else wo_b.at[c - SLOTS]

    def wo_late_copy(c):
        return pltpu.make_async_copy(wo.at[pl.ds(early, late), pl.ds(c * TILE, TILE)], wo_late(c), wo2_sem.at[c])

    small = [pltpu.make_async_copy(src, dst, in_sem.at[n])
             for n, (src, dst) in enumerate([(x_hbm, a_s), (gain_hbm, gain_s), (turn_hbm, turn_s), (base_hbm, base_s)])]
    for copy in small:
        copy.start()
    for t in range(2):
        w_copy(kv_tile(t), t).start()
    with jax.named_scope("xwait"):
        for copy in small:
            copy.wait()
    for t in range(2, 4):
        w_copy(kv_tile(t), t).start()

    gain = jnp.concatenate([gain_s[n : n + 1, :].astype(jnp.float32) for n in range(dim // HEAD)], axis=1)

    def norm(r, _):
        rows = pl.ds(pl.multiple_of(r * 16, 16), 16)
        wide = a_s[rows, :].astype(jnp.float32)
        scale = lax.rsqrt(jnp.mean(wide * wide, -1, keepdims=True) + 1e-6)
        a_s[rows, :] = (wide * scale * gain).astype(jnp.bfloat16)
        return 0

    with jax.named_scope("norm"):
        lax.fori_loop(0, own // 16, norm, 0, unroll=2)
    for t in range(4, SLOTS):
        w_copy(kv_tile(t) if t < n_kv else q_tile(jnp.int32(t - n_kv)), t).start()

    cos_b, sin_b = base_s[0, pl.ds(i, 1), :], base_s[1, pl.ds(i, 1), :]
    cos_r, sin_r = turn_s[0], turn_s[1]
    sign = jnp.where(lax.broadcasted_iota(jnp.int32, (1, HEAD), 1) < HEAD // 2, -1.0, 1.0)
    turn_s[0] = cos_b * cos_r - sin_b * sin_r
    turn_s[1] = (sin_b * cos_r + cos_b * sin_r) * sign

    def project(slot):
        return jnp.dot(a_s[...], w_s[slot], preferred_element_type=jnp.float32).astype(jnp.bfloat16)

    def turned(t):
        t = t.astype(jnp.float32)
        return (t * turn_s[0] + pltpu.roll(t, HEAD // 2, 1) * turn_s[1]).astype(jnp.bfloat16)

    def kv1(kind, p):
        return pltpu.make_async_remote_copy(
            src_ref=kv_snd.at[kind * side + p], dst_ref=kv.at[kind, x, y],
            send_sem=kv1_s.at[kind, p], recv_sem=kv1_r.at[kind, place[kind]], device_id=peer(kind, p), device_id_type=MESH)

    def kv1_in(kind, p):
        dst = kv.at[0, p, y] if kind == 0 else kv.at[1, x, p]
        return pltpu.make_async_remote_copy(
            src_ref=kv_snd.at[kind * side + p], dst_ref=dst,
            send_sem=kv1_s.at[kind, p], recv_sem=kv1_r.at[kind, p], device_id=peer(kind, p), device_id_type=MESH)

    half = side * HEAD // TILE
    heads = TILE // HEAD
    for kind in range(2):
        mine = range(kind * 2 * half, (kind + 1) * 2 * half)
        with jax.named_scope(f"kvw{kind}"):
            for t in mine:
                w_copy(kv_tile(t), t).wait()
        for t in mine:
            what, c = divmod(t - mine[0], half)
            d = project(t)
            for n in range(heads):
                h = kind * side + c * heads + n
                part = d[:, n * HEAD : (n + 1) * HEAD]
                kv_snd[h, what] = turned(part) if what == 0 else part.T
        for t in mine:
            w_copy(q_tile(jnp.int32(t + SLOTS - n_kv)), t).start()
        if kind == 0:
            with jax.named_scope("barrier"):
                pl.semaphore_wait(barrier, 2 * (side - 1))
        kv[kind, x, y] = kv_snd[kind * side + place[kind]]
        for rel in (2, 1, 3):
            kv1(kind, lax.rem(place[kind] + rel, side)).start()

    def kv2(kind, p, part, to, sem):
        some = pl.ds(part * (side // 2), side // 2)
        ref = kv.at[0, some, p] if kind == 0 else kv.at[1, p, some]
        return pltpu.make_async_remote_copy(
            src_ref=ref, dst_ref=ref, send_sem=kv2_s.at[kind, sem], recv_sem=kv2_r.at[kind, p, part],
            device_id=peer(1 - kind, to), device_id_type=MESH)

    up, down = [lax.rem(p + 1, side) for p in (y, x)], [lax.rem(p + side - 1, side) for p in (y, x)]
    direct_a = [kv2(0, y, 0, up[0], 0), kv2(0, y, 1, down[0], 2), kv2(0, y, 1, up[0], 1), kv2(0, y, 0, down[0], 3)]
    relay_a = [kv2(0, down[0], 0, up[0], 4), kv2(0, up[0], 1, down[0], 5)]
    direct_b = [kv2(1, x, part, up[1], part) for part in range(2)]
    around_b = [kv2(1, x, part, down[1], 2 + part) for part in range(2)]
    relay_b = [kv2(1, jnp.where(x == side - 1, 0, x - 1), part, 2 * side - 3 - x, 4 + part) for part in range(2)]

    def second_leg(kind):
        for rel in range(1, side):
            kv1_in(kind, lax.rem(place[kind] + rel, side)).wait_recv()
        if kind == 0:
            for copy in direct_a:
                copy.start()
        else:
            @pl.when(x < side - 1)
            def _():
                for copy in direct_b:
                    copy.start()

            @pl.when(x == 0)
            def _():
                for copy in around_b:
                    copy.start()

    def pass_on_a():
        for copy in relay_a:
            copy.wait_recv()
            copy.start()

    def pass_on_b(part):
        @pl.when(x >= side - 2)
        def _():
            relay_b[part].wait_recv()
            relay_b[part].start()

    def q_out(c):
        kind, rel, p, g = q_group(c)
        at = jnp.where(kind == 0, x, y)
        px, py = jnp.where(kind == 0, p, x), jnp.where(kind == 0, y, p)
        return rel, pltpu.make_async_remote_copy(
            src_ref=q_snd.at[c], dst_ref=q.at[kind, at], send_sem=q_s.at[c], recv_sem=q_r.at[kind, at],
            device_id=dev(px, py), device_id_type=MESH)

    def queries(c, _):
        slots = [lax.rem(c * per + j + n_kv, SLOTS) for j in range(per)]
        with jax.named_scope("qw"):
            for j in range(per):
                w_copy(q_tile(c * per + j), slots[j]).wait()

        @pl.when(c == 2 * side - 2)
        def _():
            wo_early(0).start()

        @pl.when(c == 2 * side - 1)
        def _():
            for n in range(1, 8):
                wo_early(n).start()

        @pl.when(c == 2)
        @jax.named_scope("leg1")
        def _():
            second_leg(1)

        @pl.when(c == side)
        @jax.named_scope("pass0")
        def _():
            pass_on_a()

        for j in range(per):
            d = project(slots[j])
            for n in range(heads):
                q_snd[c, j * heads + n] = turned(d[:, n * HEAD : (n + 1) * HEAD])

        rel, copy = q_out(c)

        @pl.when(rel != 0)
        def _():
            copy.start()

        @pl.when(rel == 0)
        def _():
            kind = lax.div(c, side)
            q[kind, jnp.where(kind == 0, x, y)] = q_snd[c]

        @pl.when(c == 0)
        @jax.named_scope("leg0")
        def _():
            second_leg(0)

        for j in range(per):
            u = c * per + j + SLOTS

            @pl.when(u < n_q)
            def _():
                w_copy(q_tile(u), slots[j]).start()

        return 0

    with jax.named_scope("queries"):
        lax.fori_loop(0, 2 * side, queries, 0)

    again = pltpu.make_async_copy(x_hbm, a_s, in_sem.at[0])
    again.start()

    with jax.named_scope("pass1"):
        pass_on_b(0)
    with jax.named_scope("pass2"):
        pass_on_b(1)

    span = side * own
    strip = 2 * own
    ones = jnp.ones((8, span), jnp.bfloat16)

    def o_out(kind, idx):
        px, py = jnp.where(kind == 0, idx, x), jnp.where(kind == 0, y, idx)
        return pltpu.make_async_remote_copy(
            src_ref=q_snd.at[kind * side + idx], dst_ref=o.at[kind * side + jnp.where(kind == 0, x, y)], send_sem=o_s.at[kind, idx],
            recv_sem=o_r.at[kind * side + jnp.where(kind == 0, x, y)], device_id=dev(px, py), device_id_type=MESH)

    def work(kind, idx, parts, off):
        def scores(n):
            rows = q[kind, idx, 2 * n : 2 * n + 2].reshape(strip, HEAD)
            top = None
            for kk in range(parts):
                keys = kv[kind, kk, :, 0].reshape(span, HEAD)
                s = lax.dot_general(keys, rows, (((1,), (1,)), ((), ())), preferred_element_type=jnp.float32)
                if kk == parts - 1:
                    token = lax.rem(lax.broadcasted_iota(jnp.int32, (1, strip), 1), own) + off
                    s = jnp.where(token >= lax.broadcasted_iota(jnp.int32, (span, strip), 0), s, HIDDEN)
                s_s[n % 2, pl.ds(kk * span, span), :] = s
                m = s.max(axis=0, keepdims=True)
                top = m if top is None else jnp.maximum(top, m)
            return top

        def finish(n, top):
            acc = None
            for kk in range(parts):
                p = jnp.exp2((s_s[n % 2, pl.ds(kk * span, span), :] - top) * e).astype(jnp.bfloat16)
                values = jnp.concatenate([kv[kind, kk, b, 1] for b in range(side)], axis=1)
                values = jnp.concatenate([values, ones], axis=0)
                part = jnp.dot(values, p, preferred_element_type=jnp.float32)
                acc = part if acc is None else acc + part
            res = acc[:HEAD] * (1 / acc[HEAD : HEAD + 1])
            for m in range(2):
                q_snd[kind * side + idx, 2 * n + m] = res[:, m * own : (m + 1) * own].T.astype(jnp.bfloat16)

        top = scores(0)
        for n in range(group // 2):
            nxt = scores(n + 1) if n + 1 < group // 2 else None
            finish(n, top)
            top = nxt

    def block(kind, idx, parts, off):
        for c in range(1, side + 1):
            @pl.when(parts == c)
            def _():
                with jax.named_scope(f"work{c}"):
                    work(kind, idx, c, off)

        mine = jnp.where(kind == 0, x, y)

        @pl.when(idx != mine)
        def _():
            o_out(kind, idx).start()

        @pl.when(idx == mine)
        def _():
            o[kind * side + mine] = q_snd[kind * side + idx]

    def arrived(kind):
        for rel in range(1, side):
            p = lax.rem(place[kind] + rel, side)
            with jax.named_scope(f"arrq{kind}"):
                pltpu.make_async_remote_copy(
                    src_ref=q.at[kind, p], dst_ref=q.at[kind, p], send_sem=q_s.at[0], recv_sem=q_r.at[kind, p],
                    device_id=peer(kind, p), device_id_type=MESH).wait_recv()
        with jax.named_scope(f"arrk{kind}"):
            if kind == 0:
                across = lax.rem(y + 2, side)
                for p, part in [(down[0], 1), (up[0], 0), (across, 0), (across, 1)]:
                    kv2(0, p, part, p, 0).wait_recv()
            else:
                for part in range(2):
                    @pl.when((x == 1) | (x == 2))
                    def _():
                        kv2(1, 0, part, 0, 0).wait_recv()

                    @pl.when(x == side - 1)
                    def _():
                        kv2(1, 1, part, 1, 0).wait_recv()
                        kv2(1, 2, part, 2, 0).wait_recv()
        with jax.named_scope(f"qsent{kind}"):
            for c in range(kind * side, (kind + 1) * side - 1):
                q_out(jnp.int32(c))[1].wait_send()

    def attention(n, _):
        others = 2 * (side - 1)
        kind = jnp.where(n < others, lax.div(n, side - 1), n - others)
        r = jnp.where(n < others, lax.rem(n, side - 1), side - 1)
        idx = lax.rem(jnp.where(kind == 0, x, y) + r + 1, side)

        for m in range(side):
            @pl.when(n == m)
            def _():
                for c in range(m * strips // side, (m + 1) * strips // side):
                    wo_late_copy(strips - 1 - c).start()

        @pl.when(n == 0)
        def _():
            arrived(0)

        @pl.when(n == side - 1)
        def _():
            arrived(1)

        block(kind, idx, jnp.where(kind == 0, idx, x) + 1, own * jnp.where(kind == 0, y, idx))
        return 0

    lax.fori_loop(0, 2 * side, attention, 0)

    def out_copy(c):
        at = pl.ds(c * (dim // 4), dim // 4)
        return pltpu.make_async_copy(a_s.at[:, at], out_hbm.at[:, at], out_sem.at[c])

    def wait_o(g):
        kind, p = divmod(g, side)

        @pl.when(p != place[kind])
        @jax.named_scope(f"owait{g}")
        def _():
            pltpu.make_async_remote_copy(
                src_ref=o.at[g], dst_ref=o.at[g], send_sem=o_s.at[0, 0], recv_sem=o_r.at[g],
                device_id=peer(kind, jnp.int32(p)), device_id_type=MESH).wait_recv()

    def rows_of(groups):
        return jnp.concatenate([o[g, n] for g in groups for n in range(group)], axis=1)

    def tile(c, rows):
        return w_s[c, rows, :] if c < SLOTS else wo_b[c - SLOTS, rows, :]

    order = [strips - 1 - c for c in range(strips)]
    for g in range(side):
        wait_o(g)
    with jax.named_scope("woa"):
        for c in range(8):
            wo_early(c).wait()
    with jax.named_scope("wob"):
        for c in order:
            wo_late_copy(c).wait()
    first, second = rows_of(range(EARLY)), rows_of(range(EARLY, side))
    middle = (side - EARLY) * chunk
    for c in order:
        part = jnp.dot(first, wo_a[:, c * TILE : (c + 1) * TILE], preferred_element_type=jnp.float32)
        part += jnp.dot(second, tile(c, pl.ds(0, middle)), preferred_element_type=jnp.float32)
        s_s[0, pl.ds(c * own, own), :] = part
    again.wait()
    for g in range(side, 2 * side):
        wait_o(g)
    rows = rows_of(range(side, 2 * side))
    for n in range(4):
        for c in order[n * strips // 4 : (n + 1) * strips // 4]:
            at = slice(c * TILE, (c + 1) * TILE)
            part = s_s[0, pl.ds(c * own, own), :]
            part += jnp.dot(rows, tile(c, pl.ds(middle, late - middle)), preferred_element_type=jnp.float32)
            a_s[:, at] = (a_s[:, at].astype(jnp.float32) + part).astype(jnp.bfloat16)
        out_copy(3 - n).start()

    ending = jax.named_scope("end")
    ending.__enter__()
    for kind in range(2):
        for rel in range(1, side):
            p = lax.rem(place[kind] + rel, side)
            kv1(kind, p).wait_send()
            o_out(kind, p).wait_send()
    for copy in direct_a + relay_a:
        copy.wait_send()

    @pl.when(x < side - 1)
    def _():
        for copy in direct_b:
            copy.wait_send()

    @pl.when(x == 0)
    def _():
        for copy in around_b:
            copy.wait_send()

    @pl.when(x >= side - 2)
    def _():
        for copy in relay_b:
            copy.wait_send()

    for c in range(4):
        out_copy(c).wait()
    ending.__exit__(None, None, None)


def solution(mesh):
    side = math.isqrt(mesh.shape["sp"])

    def step(x, gain, wq, wk, wv, wo):
        own, dim = x.shape
        group = wq.shape[1] // wk.shape[1]
        half, places = HEAD // 2, mesh.shape["sp"]
        rate = np.tile(np.float32(THETA) ** (-np.arange(half, dtype=np.float32) / half), 2).astype(np.float64)

        def turns(tokens):
            angle = tokens[:, None] * rate
            return jnp.asarray(np.stack([np.cos(angle), np.sin(angle)]).astype(np.float32))

        turn, base = turns(np.arange(own)), turns(np.arange(places) * own)
        blocks, chunk, bf = 2 * side, group * HEAD, jnp.bfloat16
        dma = pltpu.SemaphoreType.DMA
        hbm = pl.BlockSpec(memory_space=pl.ANY)
        return pl.pallas_call(
            functools.partial(_kernel, side, own, dim, group),
            out_shape=jax.ShapeDtypeStruct((own, dim), bf),
            in_specs=[hbm] * 8,
            out_specs=hbm,
            scratch_shapes=[
                pltpu.VMEM((dim // HEAD, HEAD), bf), pltpu.VMEM((2, own, HEAD), jnp.float32), pltpu.VMEM((2, places, HEAD), jnp.float32),
                pltpu.VMEM((own, dim), bf), pltpu.VMEM((SLOTS, dim, TILE), bf),
                pltpu.VMEM((EARLY * chunk, dim), bf), pltpu.VMEM((dim // TILE - SLOTS, (blocks - EARLY) * chunk, TILE), bf),
                pltpu.VMEM((blocks, 2, HEAD, HEAD), bf), pltpu.VMEM((2, side, side, 2, HEAD, HEAD), bf),
                pltpu.VMEM((blocks, group, own, HEAD), bf), pltpu.VMEM((2, side, group, own, HEAD), bf),
                pltpu.VMEM((blocks, group, own, HEAD), bf),
                pltpu.VMEM((2, side * side * own, 2 * own), jnp.float32),
                dma((4,)), dma((SLOTS,)), dma((8,)), dma((dim // TILE,)), dma((4,)),
                dma((2, side)), dma((2, side)), dma((2, 6)), dma((2, side, 2)),
                dma((blocks,)), dma((2, side)), dma((2, side)), dma((blocks,)),
            ],
            compiler_params=pltpu.CompilerParams(collective_id=0, has_side_effects=True, vmem_limit_bytes=67043328),
        )(x, gain.reshape(dim // HEAD, HEAD), turn, base, wq, wk, wv, wo)

    tokens, whole = P(("dp", "sp"), None), P(None, None)
    return jax.shard_map(
        step,
        mesh=mesh,
        in_specs=(tokens, P(None), whole, whole, whole, whole),
        out_specs=tokens,
        check_vma=False,
    )
```

```python
import functools
import math

import jax
import jax.numpy as jnp
import numpy as np
from jax import lax
from jax.experimental import pallas as pl
from jax.experimental.pallas import tpu as pltpu
from jax.sharding import PartitionSpec as P

HEAD = 128
THETA = 10000
LOG2E = 1.4426950408889634
HIDDEN = -2e30
MESH = pl.DeviceIdType.MESH
TILE = 256
SLOTS = 10
EARLY = 3


def _kernel(side, own, dim, group, x_hbm, gain_hbm, turn_hbm, base_hbm, wq, wk, wv, wo, out_ref,
            gain_s, turn_s, base_s, a_s, w_s, wo_a, wo_b, kv, q_snd, q, o, s_s,
            in_sem, w_sem, wo_sem, wo2_sem, kv1_s, kv1_r, kv2_s, kv2_r, q_s, q_r, o_s, o_r):
    i = lax.axis_index("sp")
    x, y = lax.div(i, side), lax.rem(i, side)
    place = (x, y)
    chunk = group * HEAD
    per = chunk // TILE
    n_kv = 2 * (2 * side) * HEAD // TILE
    n_q = 2 * side * per
    strips = dim // TILE
    early = EARLY * chunk
    late = 2 * side * chunk - early
    e = HEAD**-0.5 * LOG2E

    def dev(px, py):
        return {"sp": px * side + py}

    def peer(kind, p):
        return dev(p, y) if kind == 0 else dev(x, p)

    barrier = pltpu.get_barrier_semaphore()
    for kind in range(2):
        for rel in range(1, side):
            pl.semaphore_signal(barrier, inc=1, device_id=peer(kind, lax.rem(place[kind] + rel, side)), device_id_type=MESH)

    def kv_tile(t):
        half = side * HEAD // TILE
        kind, r = divmod(t, 2 * half)
        what, c = divmod(r, half)
        return (wk, wv)[what].at[:, pl.ds((kind * half + c) * TILE, TILE)]

    def q_group(c):
        kind, s = lax.div(c, side), lax.rem(c, side)
        rel = jnp.where(s == 0, 2, jnp.where(s == 1, 1, lax.rem(s + 1, side)))
        p = lax.rem(jnp.where(kind == 0, x, y) + rel, side)
        return kind, rel, p, kind * side + p

    def q_tile(u):
        c, j = lax.div(u, per), lax.rem(u, per)
        _, _, _, g = q_group(c)
        return wq.at[:, pl.ds(pl.multiple_of(g * chunk + j * TILE, TILE), TILE)]

    def w_copy(src, slot):
        return pltpu.make_async_copy(src, w_s.at[slot], w_sem.at[slot])

    def wo_early(c):
        at = pl.ds(c * (dim // 8), dim // 8)
        return pltpu.make_async_copy(wo.at[pl.ds(0, early), at], wo_a.at[:, at], wo_sem.at[c])

    def wo_late(c):
        return w_s.at[c, pl.ds(0, late)] if c < SLOTS else wo_b.at[c - SLOTS]

    def wo_late_copy(c):
        return pltpu.make_async_copy(wo.at[pl.ds(early, late), pl.ds(c * TILE, TILE)], wo_late(c), wo2_sem.at[c])

    small = [pltpu.make_async_copy(src, dst, in_sem.at[n])
             for n, (src, dst) in enumerate([(x_hbm, a_s), (gain_hbm, gain_s), (turn_hbm, turn_s), (base_hbm, base_s)])]
    for copy in small:
        copy.start()
    for t in range(2):
        w_copy(kv_tile(t), t).start()
    with jax.named_scope("xwait"):
        for copy in small:
            copy.wait()
    for t in range(2, 4):
        w_copy(kv_tile(t), t).start()

    gain = jnp.concatenate([gain_s[n : n + 1, :].astype(jnp.float32) for n in range(dim // HEAD)], axis=1)

    def norm(r, _):
        rows = pl.ds(pl.multiple_of(r * 16, 16), 16)
        wide = a_s[rows, :].astype(jnp.float32)
        scale = lax.rsqrt(jnp.mean(wide * wide, -1, keepdims=True) + 1e-6)
        a_s[rows, :] = (wide * scale * gain).astype(jnp.bfloat16)
        return 0

    with jax.named_scope("norm"):
        lax.fori_loop(0, own // 16, norm, 0, unroll=2)
    for t in range(4, SLOTS):
        w_copy(kv_tile(t) if t < n_kv else q_tile(jnp.int32(t - n_kv)), t).start()

    cos_b, sin_b = base_s[0, pl.ds(i, 1), :], base_s[1, pl.ds(i, 1), :]
    cos_r, sin_r = turn_s[0], turn_s[1]
    sign = jnp.where(lax.broadcasted_iota(jnp.int32, (1, HEAD), 1) < HEAD // 2, -1.0, 1.0)
    turn_s[0] = cos_b * cos_r - sin_b * sin_r
    turn_s[1] = (sin_b * cos_r + cos_b * sin_r) * sign

    def project(slot):
        return jnp.dot(a_s[...], w_s[slot], preferred_element_type=jnp.float32).astype(jnp.bfloat16)

    def turned(t):
        t = t.astype(jnp.float32)
        return (t * turn_s[0] + pltpu.roll(t, HEAD // 2, 1) * turn_s[1]).astype(jnp.bfloat16)

    def kv_rows(kind, p):
        return pl.ds(pl.multiple_of((kind * side + p) * HEAD, HEAD), HEAD)

    def kv1(kind, p):
        return pltpu.make_async_remote_copy(
            src_ref=wo_b.at[0, kv_rows(kind, p)], dst_ref=kv.at[kind, x, y],
            send_sem=kv1_s.at[kind, p], recv_sem=kv1_r.at[kind, place[kind]], device_id=peer(kind, p), device_id_type=MESH)

    def kv1_in(kind, p):
        dst = kv.at[0, p, y] if kind == 0 else kv.at[1, x, p]
        return pltpu.make_async_remote_copy(
            src_ref=wo_b.at[0, kv_rows(kind, p)], dst_ref=dst,
            send_sem=kv1_s.at[kind, p], recv_sem=kv1_r.at[kind, p], device_id=peer(kind, p), device_id_type=MESH)

    half = side * HEAD // TILE
    heads = TILE // HEAD
    for kind in range(2):
        mine = range(kind * 2 * half, (kind + 1) * 2 * half)
        with jax.named_scope(f"kvw{kind}"):
            for t in mine:
                w_copy(kv_tile(t), t).wait()
        for t in mine:
            what, c = divmod(t - mine[0], half)
            d = project(t)
            for n in range(heads):
                h = kind * side + c * heads + n
                part = d[:, n * HEAD : (n + 1) * HEAD]
                wo_b[0, h * HEAD : (h + 1) * HEAD, what * HEAD : (what + 1) * HEAD] = turned(part) if what == 0 else part.T
        for t in mine:
            w_copy(q_tile(jnp.int32(t + SLOTS - n_kv)), t).start()
        if kind == 0:
            with jax.named_scope("barrier"):
                pl.semaphore_wait(barrier, 2 * (side - 1))
        kv[kind, x, y] = wo_b[0, kv_rows(kind, place[kind]), :]
        for rel in (2, 1, 3):
            kv1(kind, lax.rem(place[kind] + rel, side)).start()

    def kv2(kind, p, part, to, sem):
        some = pl.ds(part * (side // 2), side // 2)
        ref = kv.at[0, some, p] if kind == 0 else kv.at[1, p, some]
        return pltpu.make_async_remote_copy(
            src_ref=ref, dst_ref=ref, send_sem=kv2_s.at[kind, sem], recv_sem=kv2_r.at[kind, p, part],
            device_id=peer(1 - kind, to), device_id_type=MESH)

    up, down = [lax.rem(p + 1, side) for p in (y, x)], [lax.rem(p + side - 1, side) for p in (y, x)]
    direct_a = [kv2(0, y, 0, up[0], 0), kv2(0, y, 1, down[0], 2), kv2(0, y, 1, up[0], 1), kv2(0, y, 0, down[0], 3)]
    relay_a = [kv2(0, down[0], 0, up[0], 4), kv2(0, up[0], 1, down[0], 5)]
    direct_b = [kv2(1, x, part, up[1], part) for part in range(2)]
    around_b = [kv2(1, x, part, down[1], 2 + part) for part in range(2)]
    relay_b = [kv2(1, jnp.where(x == side - 1, 0, x - 1), part, 2 * side - 3 - x, 4 + part) for part in range(2)]

    def second_leg(kind):
        for rel in range(1, side):
            kv1_in(kind, lax.rem(place[kind] + rel, side)).wait_recv()
        if kind == 0:
            for copy in direct_a:
                copy.start()
        else:
            @pl.when(x < side - 1)
            def _():
                for copy in direct_b:
                    copy.start()

            @pl.when(x == 0)
            def _():
                for copy in around_b:
                    copy.start()

    def pass_on_a():
        for copy in relay_a:
            copy.wait_recv()
            copy.start()

    def pass_on_b(part):
        @pl.when(x >= side - 2)
        def _():
            relay_b[part].wait_recv()
            relay_b[part].start()

    def q_out(c):
        kind, rel, p, g = q_group(c)
        at = jnp.where(kind == 0, x, y)
        px, py = jnp.where(kind == 0, p, x), jnp.where(kind == 0, y, p)
        return rel, pltpu.make_async_remote_copy(
            src_ref=q_snd.at[c], dst_ref=q.at[kind, at], send_sem=q_s.at[c], recv_sem=q_r.at[kind, at],
            device_id=dev(px, py), device_id_type=MESH)

    def queries(c, _):
        slots = [lax.rem(c * per + j + n_kv, SLOTS) for j in range(per)]
        with jax.named_scope("qw"):
            for j in range(per):
                w_copy(q_tile(c * per + j), slots[j]).wait()

        @pl.when(c == 2 * side - 2)
        def _():
            wo_early(0).start()

        @pl.when(c == 2 * side - 1)
        def _():
            for n in range(1, 8):
                wo_early(n).start()

        @pl.when(c == 2)
        @jax.named_scope("leg1")
        def _():
            second_leg(1)

        @pl.when(c == side)
        @jax.named_scope("pass0")
        def _():
            pass_on_a()

        for j in range(per):
            d = project(slots[j])
            for n in range(heads):
                q_snd[c, j * heads + n] = turned(d[:, n * HEAD : (n + 1) * HEAD])

        rel, copy = q_out(c)

        @pl.when(rel != 0)
        def _():
            copy.start()

        @pl.when(rel == 0)
        def _():
            kind = lax.div(c, side)
            q[kind, jnp.where(kind == 0, x, y)] = q_snd[c]

        @pl.when(c == 0)
        @jax.named_scope("leg0")
        def _():
            second_leg(0)

        for j in range(per):
            u = c * per + j + SLOTS

            @pl.when(u < n_q)
            def _():
                w_copy(q_tile(u), slots[j]).start()

        return 0

    with jax.named_scope("queries"):
        lax.fori_loop(0, 2 * side, queries, 0)

    again = pltpu.make_async_copy(x_hbm, a_s, in_sem.at[0])
    again.start()

    for kind in range(2):
        for rel in range(1, side):
            kv1(kind, lax.rem(place[kind] + rel, side)).wait_send()
    with jax.named_scope("pass1"):
        pass_on_b(0)
    with jax.named_scope("pass2"):
        pass_on_b(1)

    span = side * own
    strip = 2 * own

    def o_out(kind, idx):
        px, py = jnp.where(kind == 0, idx, x), jnp.where(kind == 0, y, idx)
        return pltpu.make_async_remote_copy(
            src_ref=q_snd.at[kind * side + idx], dst_ref=o.at[kind * side + jnp.where(kind == 0, x, y)], send_sem=o_s.at[kind, idx],
            recv_sem=o_r.at[kind * side + jnp.where(kind == 0, x, y)], device_id=dev(px, py), device_id_type=MESH)

    def work(kind, idx, parts, last):
        blocks = [side] * (parts - 1) + [last]

        def scores(n):
            rows = q[kind, idx, 2 * n : 2 * n + 2].reshape(strip, HEAD)
            top = None
            for kk, some in enumerate(blocks):
                keys = kv[kind, kk, 0:some, :, 0:HEAD].reshape(some * own, HEAD)
                s = lax.dot_general(keys, rows, (((1,), (1,)), ((), ())), preferred_element_type=jnp.float32)
                pieces = [s]
                if kk == parts - 1:
                    token = lax.rem(lax.broadcasted_iota(jnp.int32, (1, strip), 1), own)
                    cut = s[(some - 1) * own :]
                    cut = jnp.where(token >= lax.broadcasted_iota(jnp.int32, (own, strip), 0), cut, HIDDEN)
                    pieces = [s[: (some - 1) * own], cut] if some > 1 else [cut]
                at = kk * span
                for piece in pieces:
                    s_s[n % 2, pl.ds(at, piece.shape[0]), :] = piece
                    at += piece.shape[0]
                    m = piece.max(axis=0, keepdims=True)
                    top = m if top is None else jnp.maximum(top, m)
            return top

        def finish(n, top):
            acc = None
            for kk, some in enumerate(blocks):
                p = jnp.exp2((s_s[n % 2, pl.ds(kk * span, some * own), :] - top) * e).astype(jnp.bfloat16)
                values = jnp.concatenate([kv[kind, kk, b, :, HEAD:] for b in range(some)], axis=1)
                values = jnp.concatenate([values, jnp.ones((8, some * own), jnp.bfloat16)], axis=0)
                part = jnp.dot(values, p, preferred_element_type=jnp.float32)
                acc = part if acc is None else acc + part
            res = acc[:HEAD] * (1 / acc[HEAD : HEAD + 1])
            for m in range(2):
                q_snd[kind * side + idx, 2 * n + m] = res[:, m * own : (m + 1) * own].T.astype(jnp.bfloat16)

        top = scores(0)
        for n in range(group // 2):
            nxt = scores(n + 1) if n + 1 < group // 2 else None
            finish(n, top)
            top = nxt

    def block(kind, idx, parts, last):
        for c in range(1, side + 1):
            for m in range(1, side + 1):
                @pl.when((parts == c) & (last == m))
                def _():
                    with jax.named_scope(f"work{c}{m}"):
                        work(kind, idx, c, m)

        mine = jnp.where(kind == 0, x, y)

        @pl.when(idx != mine)
        def _():
            o_out(kind, idx).start()

        @pl.when(idx == mine)
        def _():
            o[kind * side + mine] = q_snd[kind * side + idx]

    def arrived(kind):
        for rel in range(1, side):
            p = lax.rem(place[kind] + rel, side)
            with jax.named_scope(f"arrq{kind}"):
                pltpu.make_async_remote_copy(
                    src_ref=q.at[kind, p], dst_ref=q.at[kind, p], send_sem=q_s.at[0], recv_sem=q_r.at[kind, p],
                    device_id=peer(kind, p), device_id_type=MESH).wait_recv()
        with jax.named_scope(f"arrk{kind}"):
            if kind == 0:
                across = lax.rem(y + 2, side)
                for p, part in [(down[0], 1), (up[0], 0), (across, 0), (across, 1)]:
                    kv2(0, p, part, p, 0).wait_recv()
            else:
                for part in range(2):
                    @pl.when((x == 1) | (x == 2))
                    def _():
                        kv2(1, 0, part, 0, 0).wait_recv()

                    @pl.when(x == side - 1)
                    def _():
                        kv2(1, 1, part, 1, 0).wait_recv()
                        kv2(1, 2, part, 2, 0).wait_recv()
        with jax.named_scope(f"qsent{kind}"):
            for c in range(kind * side, (kind + 1) * side - 1):
                q_out(jnp.int32(c))[1].wait_send()

    def attention(n, _):
        others = 2 * (side - 1)
        kind = jnp.where(n < others, lax.div(n, side - 1), n - others)
        r = jnp.where(n < others, lax.rem(n, side - 1), side - 1)
        idx = lax.rem(jnp.where(kind == 0, x, y) + r + 1, side)

        for m in range(side):
            @pl.when(n == m)
            def _():
                for c in range(m * strips // side, (m + 1) * strips // side):
                    wo_late_copy(strips - 1 - c).start()

        @pl.when(n == 0)
        def _():
            arrived(0)

        @pl.when(n == side - 1)
        def _():
            arrived(1)

        block(kind, idx, jnp.where(kind == 0, idx, x) + 1, jnp.where(kind == 0, y, idx) + 1)
        return 0

    lax.fori_loop(0, 2 * side, attention, 0)

    def wait_o(g):
        kind, p = divmod(g, side)

        @pl.when(p != place[kind])
        @jax.named_scope(f"owait{g}")
        def _():
            pltpu.make_async_remote_copy(
                src_ref=o.at[g], dst_ref=o.at[g], send_sem=o_s.at[0, 0], recv_sem=o_r.at[g],
                device_id=peer(kind, jnp.int32(p)), device_id_type=MESH).wait_recv()

    def rows_of(groups):
        return jnp.concatenate([o[g, n] for g in groups for n in range(group)], axis=1)

    def tile(c, rows):
        return w_s[c, rows, :] if c < SLOTS else wo_b[c - SLOTS, rows, :]

    order = [strips - 1 - c for c in range(strips)]
    for g in range(side):
        wait_o(g)
    with jax.named_scope("woa"):
        for c in range(8):
            wo_early(c).wait()
    with jax.named_scope("wob"):
        for c in order:
            wo_late_copy(c).wait()
    first, second = rows_of(range(EARLY)), rows_of(range(EARLY, side))
    middle = (side - EARLY) * chunk
    for c in order:
        part = jnp.dot(first, wo_a[:, c * TILE : (c + 1) * TILE], preferred_element_type=jnp.float32)
        part += jnp.dot(second, tile(c, pl.ds(0, middle)), preferred_element_type=jnp.float32)
        s_s[0, pl.ds(c * own, own), :] = part
    again.wait()
    for g in range(side, 2 * side):
        wait_o(g)
    rows = rows_of(range(side, 2 * side))
    for n in range(4):
        for c in order[n * strips // 4 : (n + 1) * strips // 4]:
            at = slice(c * TILE, (c + 1) * TILE)
            part = s_s[0, pl.ds(c * own, own), :]
            part += jnp.dot(rows, tile(c, pl.ds(middle, late - middle)), preferred_element_type=jnp.float32)
            out_ref[:, at] = (a_s[:, at].astype(jnp.float32) + part).astype(jnp.bfloat16)

    ending = jax.named_scope("end")
    ending.__enter__()
    for kind in range(2):
        for rel in range(1, side):
            p = lax.rem(place[kind] + rel, side)
            o_out(kind, p).wait_send()
    for copy in direct_a + relay_a:
        copy.wait_send()

    @pl.when(x < side - 1)
    def _():
        for copy in direct_b:
            copy.wait_send()

    @pl.when(x == 0)
    def _():
        for copy in around_b:
            copy.wait_send()

    @pl.when(x >= side - 2)
    def _():
        for copy in relay_b:
            copy.wait_send()

    ending.__exit__(None, None, None)


def solution(mesh):
    side = math.isqrt(mesh.shape["sp"])

    def step(x, gain, wq, wk, wv, wo):
        own, dim = x.shape
        group = wq.shape[1] // wk.shape[1]
        half, places = HEAD // 2, mesh.shape["sp"]
        rate = np.tile(np.float32(THETA) ** (-np.arange(half, dtype=np.float32) / half), 2).astype(np.float64)

        def turns(tokens):
            angle = tokens[:, None] * rate
            return jnp.asarray(np.stack([np.cos(angle), np.sin(angle)]).astype(np.float32))

        turn, base = turns(np.arange(own)), turns(np.arange(places) * own)
        blocks, chunk, bf = 2 * side, group * HEAD, jnp.bfloat16
        dma = pltpu.SemaphoreType.DMA
        hbm = pl.BlockSpec(memory_space=pl.ANY)
        return pl.pallas_call(
            functools.partial(_kernel, side, own, dim, group),
            out_shape=pltpu.VMEM((own, dim), bf),
            in_specs=[hbm] * 8,
            out_specs=pl.BlockSpec(memory_space=pltpu.VMEM),
            scratch_shapes=[
                pltpu.VMEM((dim // HEAD, HEAD), bf), pltpu.VMEM((2, own, HEAD), jnp.float32), pltpu.VMEM((2, places, HEAD), jnp.float32),
                pltpu.VMEM((own, dim), bf), pltpu.VMEM((SLOTS, dim, TILE), bf),
                pltpu.VMEM((EARLY * chunk, dim), bf), pltpu.VMEM((dim // TILE - SLOTS, (blocks - EARLY) * chunk, TILE), bf),
                pltpu.VMEM((2, side, side, own, 2 * HEAD), bf),
                pltpu.VMEM((blocks, group, own, HEAD), bf), pltpu.VMEM((2, side, group, own, HEAD), bf),
                pltpu.VMEM((blocks, group, own, HEAD), bf),
                pltpu.VMEM((2, side * side * own, 2 * own), jnp.float32),
                dma((4,)), dma((SLOTS,)), dma((8,)), dma((dim // TILE,)),
                dma((2, side)), dma((2, side)), dma((2, 6)), dma((2, side, 2)),
                dma((blocks,)), dma((2, side)), dma((2, side)), dma((blocks,)),
            ],
            compiler_params=pltpu.CompilerParams(collective_id=0, has_side_effects=True, vmem_limit_bytes=65900000),
        )(x, gain.reshape(dim // HEAD, HEAD), turn, base, wq, wk, wv, wo)

    tokens, whole = P(("dp", "sp"), None), P(None, None)
    return jax.shard_map(
        step,
        mesh=mesh,
        in_specs=(tokens, P(None), whole, whole, whole, whole),
        out_specs=tokens,
        check_vma=False,
    )
```
